256 devices in a mesh: a3: 8 (over z), a2: 4 (over y), a1: 8 (over x, core).
Axes of the slice: x: 4, y: 4, z: 8, core: 2. Of those that a mesh axis runs over, the one named last changes fastest.
Arguments:
- tensor: bfloat16 [384, 1024, 1024], P('a1', 'a2', 'a3')
- u_time: float32 [384, 48], replicated
- u_height: float32 [1024, 128], replicated
- u_width: float32 [1024, 128], replicated
Outputs:
- output 1: float32 [384, 48], replicated
- output 2: float32 [1024, 128], replicated
- output 3: float32 [1024, 128], replicated
- output 4: float32 [48, 128, 128], P('a1', 'a2', 'a3')
- output 5: float32 [], replicated
All inputs are finite; a program needn't handle non-finite values.
Results may differ from the reference program's by a relative error of at most 0.00243.
Values are sent between devices in bfloat16 or wider.
A program may use at most 768 MiB of HBM per device.

```python
import jax
import jax.numpy as jnp
from jax import lax

FRAMES = 384
GRID_H = 1024
GRID_W = 1024
RANK_T = 48
RANK_H = 128
RANK_W = 128
SIGNAL_RANK = 8


def setup_inputs(seed: int = 0) -> dict:
    key_list = jax.random.split(jax.random.key(seed), 8)
    fac_t = jax.random.normal(key_list[0], (FRAMES, SIGNAL_RANK), jnp.float32)
    fac_h = jax.random.normal(key_list[1], (GRID_H, SIGNAL_RANK), jnp.float32)
    fac_w = jax.random.normal(key_list[2], (GRID_W, SIGNAL_RANK), jnp.float32)
    weights = jax.random.uniform(key_list[3], (SIGNAL_RANK,), jnp.float32, 0.5, 1.5) * SIGNAL_RANK ** -0.5

    def one_frame(frame_idx):
        noise_map = jax.random.normal(jax.random.fold_in(key_list[4], frame_idx), (GRID_H, GRID_W), jnp.float32)
        signal = jnp.dot(fac_h * (fac_t[frame_idx] * weights), fac_w.T)
        return (signal + noise_map).astype(jnp.bfloat16)

    tensor = lax.map(one_frame, jnp.arange(FRAMES))
    u_time = jax.random.normal(key_list[5], (FRAMES, RANK_T), jnp.float32) * FRAMES ** -0.5
    u_height = jax.random.normal(key_list[6], (GRID_H, RANK_H), jnp.float32) * GRID_H ** -0.5
    u_width = jax.random.normal(key_list[7], (GRID_W, RANK_W), jnp.float32) * GRID_W ** -0.5
    return {'tensor': tensor, 'u_time': u_time, 'u_height': u_height, 'u_width': u_width}


def operand_f32(matrix):
    return matrix.astype(jnp.bfloat16).astype(jnp.float32)


def col_normalise(power_cols):
    return power_cols / jnp.sqrt(jnp.sum(power_cols * power_cols, axis=0, keepdims=True))


def gram_update(unfold, factor):
    gram_mat = jnp.dot(unfold, unfold.T, preferred_element_type=jnp.float32).astype(jnp.bfloat16)
    return col_normalise(jnp.dot(gram_mat, factor.astype(jnp.bfloat16), preferred_element_type=jnp.float32))


def reference(tensor, u_time, u_height, u_width):
    t_full = jnp.dot(tensor.reshape(FRAMES * GRID_H, GRID_W), u_width.astype(jnp.bfloat16), preferred_element_type=jnp.float32)
    t_mat = t_full.astype(jnp.bfloat16).reshape(FRAMES, GRID_H, RANK_W).astype(jnp.float32)
    y_one = jnp.einsum('ihc,hb->ibc', t_mat, operand_f32(u_height)).astype(jnp.bfloat16)
    new_time = gram_update(y_one.reshape(FRAMES, RANK_H * RANK_W), u_time)
    y_two = jnp.einsum('ihc,ia->hac', t_mat, operand_f32(new_time)).astype(jnp.bfloat16)
    new_height = gram_update(y_two.reshape(GRID_H, RANK_T * RANK_W), u_height)
    z_flat = jnp.dot(new_time.astype(jnp.bfloat16).T, tensor.reshape(FRAMES, GRID_H * GRID_W), preferred_element_type=jnp.float32)
    z_mat = z_flat.astype(jnp.bfloat16).reshape(RANK_T, GRID_H, GRID_W).astype(jnp.float32)
    y_three = jnp.einsum('ahw,hb->wab', z_mat, operand_f32(new_height)).astype(jnp.bfloat16)
    new_width = gram_update(y_three.reshape(GRID_W, RANK_T * RANK_H), u_width)
    core_tensor = jnp.einsum('wab,wc->abc', y_three.astype(jnp.float32), operand_f32(new_width))
    core_energy = jnp.sum(core_tensor * core_tensor)
    return new_time, new_height, new_width, core_tensor, core_energy
```

```python
import functools

import jax
import jax.numpy as jnp
from jax import lax
from jax.experimental import pallas as pl
from jax.experimental.pallas import tpu as pltpu
from jax.sharding import PartitionSpec as P

F32 = jnp.float32
BF16 = jnp.bfloat16
MESH = pl.DeviceIdType.MESH
NN = ((1,), (0,))
NT = ((1,), (1,))
TN = ((0,), (0,))


def dot(a, b, dims=NN):
    return lax.dot_general(a, b, (dims, ((), ())), preferred_element_type=F32)


class Net:
    def __init__(self, send_sem, recv_sem):
        self.send_sem, self.recv_sem, self.copies = send_sem, recv_sem, []

    def send(self, src, dst, device):
        k = len(self.copies)
        copy = pltpu.make_async_remote_copy(
            src_ref=src, dst_ref=dst, send_sem=self.send_sem.at[k], recv_sem=self.recv_sem.at[k], device_id=device, device_id_type=MESH
        )
        copy.start()
        self.copies.append(copy)
        return copy

    def finish(self):
        for copy in self.copies:
            copy.wait_send()


def arrive(copies):
    for copy in copies:
        copy.wait_recv()


def add_slots(buf, count):
    total = buf[0]
    for k in range(1, count):
        total = total + buf[k]
    return total


def swap16(perm, block):
    n = block.shape[-1]
    return dot(perm, block.reshape(256, n)).astype(BF16).reshape(16, 16, n)


def sweep_kernel(
    n1, n2, n3,
    x_hbm, u1_hbm, u2_hbm, u3_hbm,
    new1t_out, p2_out, sq2_out, p3_out, sq3_out, core_out, e_out,
    x, u1, u2, u3, u3_here, new1t, p2, sq2, p3, sq3, out_core, e3,
    perm, u1p, tp, rin, tb, tt, xp, xr, t2,
    y1p, y1y, y1b, y1a, gp1, g1y, g1z, p1y, p1a,
    y2o, y2y, z1, z2, zf, gp2, b0, g0, b1, g1, b2, p2x, p2z, p2c,
    y3p, y3y, y3o, y3z, gp3, c0, h0, c1, h1, c2, p3y, p3x, p3c,
    cp, cpz, e1, e2,
    send_sem, recv_sem, load_sem, store_sem,
):
    me1, me2, me3 = lax.axis_index("a1"), lax.axis_index("a2"), lax.axis_index("a3")
    core, mex, nx = lax.rem(me1, 2), me1 // 2, n1 // 2
    fl, hl, wl = x.shape
    net = Net(send_sem, recv_sem)
    stores = []

    def store(src, dst):
        stores.append(pltpu.make_async_copy(src, dst, store_sem.at[len(stores)]))
        stores[-1].start()


    def peers(me, n):
        return [lax.rem(me + d, n) for d in range(1, n)]

    peers1, peers2, peers3, peersx = peers(me1, n1), peers(me2, n2), peers(me3, n3), peers(mex, nx)

    def share(src, buf, me, ps, device):
        return [net.send(src(p), buf.at[me], device(p)) for p in ps]

    def on1(p):
        return {"a1": p}

    def on2(p):
        return {"a2": p}

    def on3(p):
        return {"a3": p}

    def onx(p):
        return {"a1": 2 * p + core}

    other = {"a1": 2 * mex + 1 - core}

    barrier = pltpu.get_barrier_semaphore()
    for ps, device in ((peers3, on3), (peers2, on2), (peers1, on1)):
        for p in ps:
            pl.semaphore_signal(barrier, inc=1, device_id=device(p), device_id_type=MESH)

    half = fl // 2
    width_here = pl.ds(pl.multiple_of(me3 * wl, wl), wl)
    loads = [
        pltpu.make_async_copy(src, dst, load_sem.at[k])
        for k, (src, dst) in enumerate(
            [
                (u3_hbm.at[width_here], u3_here),
                (x_hbm.at[pl.ds(0, half)], x.at[pl.ds(0, half)]),
                (x_hbm.at[pl.ds(half, half)], x.at[pl.ds(half, half)]),
                (u1_hbm, u1),
                (u2_hbm, u2),
                (u3_hbm, u3),
            ]
        )
    ]
    for load in loads:
        load.start()

    row = lax.broadcasted_iota(jnp.int32, (256, 256), 0)
    col = lax.broadcasted_iota(jnp.int32, (256, 256), 1)
    perm[...] = jnp.where(col == lax.rem(row, 16) * 16 + row // 16, 1.0, 0.0).astype(BF16)

    cz = tp.shape[2]
    reach = n3 // 2
    loads[0].wait()
    u3t = u3_here[...].T.astype(BF16)

    def t_frame(i, carry):
        tp[:, i] = dot(u3t, x[i], NT).reshape(n3, cz, hl)
        return carry

    hops, ch = n3 - 1, cz // 2
    way_step = (1, n3 - 1)

    def t_part(way, sub, root):
        return tp.at[root, pl.ds(sub * half, half), pl.ds(way * ch, ch)]

    def root_at(way, step):
        return lax.rem(me3 + n3 - step, n3) if way == 0 else lax.rem(me3 + step, n3)

    ring = {}

    def send_piece(way, sub, step):
        ring[way, sub, step] = net.send(
            t_part(way, sub, root_at(way, step)), rin.at[way, step - 1, sub], on3(lax.rem(me3 + way_step[way], n3))
        )

    loads[1].wait()
    lax.fori_loop(0, half, t_frame, 0, unroll=4)
    pl.semaphore_wait(barrier, n1 + n2 + n3 - 3)
    send_piece(0, 0, 1)
    send_piece(1, 0, 1)
    loads[2].wait()
    lax.fori_loop(half, fl, t_frame, 0, unroll=4)
    send_piece(0, 1, 1)
    send_piece(1, 1, 1)

    hr = hl // n1

    def x_slice(r):
        for hh in range(0, hr, 16):
            for g in range(0, fl, 16):
                rows = pl.ds(pl.multiple_of(r * hr + hh, 16), 16)
                xp[r, hh : hh + 16, g : g + 16, :] = swap16(perm[...], x[g : g + 16, rows, :])

    frames_here = pl.ds(pl.multiple_of(me1 * fl, fl), fl)
    x_copies = []
    for p in peers1:
        x_slice(p)
        x_copies.append(net.send(xp.at[p], xr.at[:, frames_here, :], on1(p)))
    x_slice(me1)
    xr[:, frames_here, :] = xp[me1]
    for load in loads[3:]:
        load.wait()
    rank1 = u1.shape[0]
    u1p[:, :rank1] = u1[...].T.astype(BF16)
    u1p[:, rank1:] = jnp.zeros((u1p.shape[0], 128 - rank1), BF16)

    for step in range(1, n3):
        for sub in (0, 1):
            for way in (0, 1):
                ring[way, sub, step].wait_recv()
                if step < hops:
                    mine = t_part(way, sub, root_at(way, step + 1))
                    mine[...] = mine[...] + rin[way, step - 1, sub]
                    send_piece(way, sub, step + 1)
    for sub in (0, 1):
        total = [t_part(way, sub, me3)[...] + rin[way, hops - 1, sub] for way in (0, 1)]
        tb[sub * half : (sub + 1) * half] = jnp.concatenate(total, axis=1).astype(BF16)
    for g in range(0, fl, 16):
        tt[:, g : g + 16, :] = swap16(perm[...], tb[g : g + 16])

    u2_here = u2[pl.ds(pl.multiple_of(me2 * hl, hl), hl), :].astype(BF16)
    y1p[...] = dot(tt[...].reshape(cz * fl, hl), u2_here).reshape(y1p.shape)
    cy, c1w = cz // n2, cz // n1
    y1_copies = share(lambda p: y1p.at[pl.ds(p * cy, cy)], y1y, me2, peers2, on2)
    y1y[me2] = y1p[pl.ds(me2 * cy, cy)]
    t_copies = [net.send(tt.at[pl.ds(p * c1w, c1w)], t2.at[:, frames_here, :], on1(p)) for p in peers1]
    t2[:, frames_here, :] = tt[pl.ds(me1 * c1w, c1w)]
    arrive(y1_copies)
    lane = lax.broadcasted_iota(jnp.int32, (cy, fl, 128), 2)
    width = 128 // n2
    y1 = None
    for q in range(n2):
        for side, turn in ((0, 1), (1, n2 - 1)):
            chain = y1y[(q + turn) % n2]
            for k in range(2, n2 + 1):
                chain = chain + y1y[(q + turn * k) % n2]
            y1 = chain if y1 is None else jnp.where(lane >= q * width + side * (width // 2), chain, y1)
    y1 = y1.astype(BF16)
    for c in range(cy):
        y1b[:, c * 128 : (c + 1) * 128] = y1[c]

    y1_all = share(lambda p: y1b, y1a, me1, peers1, on1)
    y1a[me1] = y1b[...]
    arrive(y1_all)
    gp1[...] = dot(y1b[...], y1a[...].reshape(n1 * fl, cy * 128), NT)
    tiles_c = gp1.shape[1] // 128

    def cols_of(p):
        return pl.ds(pl.multiple_of(lax.rem(p, tiles_c) * 128, 128), 128)

    copies = share(lambda p: gp1.at[:, cols_of(p)], g1y, me2, peers2, on2)
    g1y[me2] = gp1[:, cols_of(me2)]
    arrive(copies)
    g1z[me3] = add_slots(g1y, n2)
    arrive(share(lambda p: g1z.at[me3], g1z, me3, peers3, on3))
    gram = add_slots(g1z, n3).astype(BF16)
    p1y[me2] = dot(gram, u1p[cols_of(me2), :])
    arrive(share(lambda p: p1y.at[me2], p1y, me2, peers2, on2))
    p1a[me1] = add_slots(p1y, tiles_c)
    arrive(share(lambda p: p1a.at[me1], p1a, me1, peers1, on1))
    power = p1a[...].reshape(n1 * fl, 128).T[:rank1]
    new1 = power / jnp.sqrt(jnp.sum(power * power, axis=1, keepdims=True))
    new1t[...] = new1
    store(new1t, new1t_out)
    u1t = new1.astype(BF16)

    arrive(t_copies)
    for c in range(c1w):
        y2o[c * rank1 : (c + 1) * rank1] = dot(u1t, t2[c]).astype(BF16)
    y2y[me2] = y2o[...]
    y2_copies = share(lambda p: y2o, y2y, me2, peers2, on2)

    arrive(x_copies)
    for h in range(hr):
        z1[h] = dot(u1t, xr[h]).astype(BF16)
    for hh in range(0, hr, 16):
        for g in range(0, rank1, 16):
            z2[g : g + 16, hh : hh + 16, :] = swap16(perm[...], z1[hh : hh + 16, g : g + 16, :])
    ar = rank1 // n1
    z_rows = pl.ds(pl.multiple_of(me1 * hr, hr), hr)
    z_copies = [net.send(z2.at[pl.ds(p * ar, ar)], zf.at[:, z_rows, :], on1(p)) for p in peers1]
    zf[:, z_rows, :] = z2[pl.ds(me1 * ar, ar)]

    arrive(y2_copies)
    for q in range(n2):
        gp2[:, q] = dot(y2o[...], y2y[q], TN).reshape(2, hl // 2, hl)
    swap = net.send(gp2.at[1 - core], b0, other)
    arrive([swap])
    g0[...] = (gp2[core] + b0[...]).reshape(g0.shape)
    pieces2 = []
    parts = hl // 2 // n3 // 8
    for k in range(parts):
        b1[k, mex] = g0[mex, :, k]
        pieces_x = share(lambda p: g0.at[p, :, k], b1.at[k], mex, peersx, onx)
        pieces2.append(pieces_x)
    pieces_z = []
    for k in range(parts):
        arrive(pieces2[k])
        g1[:, k] = add_slots(b1.at[k], nx)
        pieces_z += share(lambda p: g1.at[p, k], b2.at[k], me3, peers3, on3)
        b2[k, me3] = g1[me3, k]
    arrive(pieces_z)
    gram = jnp.concatenate([add_slots(b2.at[k], n3) for k in range(parts)], axis=0).astype(BF16)
    p2x[mex] = dot(gram, u2[pl.ds(pl.multiple_of(mex * hl, hl), hl), :].astype(BF16))
    arrive(share(lambda p: p2x.at[mex], p2x, mex, peersx, onx))
    p2z[me3] = add_slots(p2x, nx)
    arrive(share(lambda p: p2z.at[me3], p2z, me3, peers3, on3))
    p2c[core] = p2z[...].reshape(hl // 2, 128)
    arrive([net.send(p2c.at[core], p2c.at[core], other)])
    power = p2c[...].reshape(hl, 128)
    sq2[me2] = jnp.broadcast_to(jnp.sum(power * power, axis=0, keepdims=True), (8, 128))
    p2[...] = power
    store(p2, p2_out.at[me2])
    copies = share(lambda p: sq2.at[me2], sq2, me2, peers2, on2)
    arrive(copies)
    store(sq2, sq2_out)
    norm2 = jnp.sqrt(add_slots(sq2, n2)[:1])
    u2t = (power / norm2).T.astype(BF16)

    arrive(z_copies)
    bq = 128 // n2
    for a in range(ar):
        y3p[:, a] = dot(u2t, zf[a]).reshape(n2, bq, wl)
    copies = share(lambda p: y3p.at[p], y3y, me2, peers2, on2)
    p2_copies = share(lambda p: p2, p2_out, me2, peers2, on2)
    y3y[me2] = y3p[me2]
    arrive(copies)
    y3o[...] = add_slots(y3y, n2).astype(BF16).reshape(ar * bq, wl)

    wx = wl // 2 // nx
    order = [d for k in range(1, reach) for d in (k, n3 - k)] + [reach]
    peer_of = {d: lax.rem(me3 + d, n3) for d in order}
    y3z[me3] = y3o[...]
    incoming = {n3 - d: net.send(y3o, y3z.at[me3], on3(peer_of[d])) for d in order}
    groups = [[0, 1, n3 - 1], [2, n3 - 2], [3, n3 - 3, 4]]
    pieces_x = []
    for group in groups:
        swaps = []
        for d in group:
            if d:
                arrive([incoming[d]])
            q = peer_of[d] if d else me3
            gp3[:, q] = dot(y3o[...], y3z[q], TN).reshape(2, wl // 2, wl)
            swaps.append((q, net.send(gp3.at[1 - core, q], c0.at[q], other)))
        for q, swap in swaps:
            arrive([swap])
            h0[:, q] = (gp3[core, q] + c0[q]).reshape(nx, wx, wl)
            c1[mex, q] = h0[mex, q]
            pieces_x += [net.send(h0.at[p, q], c1.at[mex, q], onx(p)) for p in peersx]
    arrive(pieces_x)
    h1[...] = add_slots(c1, nx)
    zq = n3 // n2
    copies = share(lambda p: h1.at[pl.ds(p * zq, zq)], c2, me2, peers2, on2)
    c2[me2] = h1[pl.ds(me2 * zq, zq)]
    arrive(copies)
    gram = add_slots(c2, n2).astype(BF16)
    power = jnp.zeros((wx, 128), F32)
    for q in range(zq):
        power = power + dot(gram[q], u3[pl.ds(pl.multiple_of((me2 * zq + q) * wl, wl), wl), :].astype(BF16))
    p3y[me2] = power
    arrive(share(lambda p: p3y.at[me2], p3y, me2, peers2, on2))
    p3x[mex] = add_slots(p3y, n2)
    arrive(share(lambda p: p3x.at[mex], p3x, mex, peersx, onx))
    p3c[core] = p3x[...].reshape(wl // 2, 128)
    arrive([net.send(p3c.at[core], p3c.at[core], other)])
    power = p3c[...].reshape(wl, 128)
    sq3[me3] = jnp.broadcast_to(jnp.sum(power * power, axis=0, keepdims=True), (8, 128))
    p3[...] = power
    store(p3, p3_out.at[me3])
    copies = share(lambda p: sq3.at[me3], sq3, me3, peers3, on3)
    arrive(copies)
    store(sq3, sq3_out)
    norm3 = jnp.sqrt(add_slots(sq3, n3)[:1])
    u3n = (power / norm3).T.astype(BF16)

    kk = ar * bq
    cp[...] = jnp.zeros_like(cp)
    cp[:, :, :kk] = dot(u3n, y3o[...], NT).reshape(n3, cz, kk)
    copies = share(lambda p: cp.at[p], cpz, me3, peers3, on3)
    p3_copies = share(lambda p: p3, p3_out, me3, peers3, on3)
    cpz[me3] = cp[me3]
    arrive(copies)
    total = add_slots(cpz, n3)
    out_core[...] = total
    store(out_core, core_out)
    e1[me1] = jnp.broadcast_to(jnp.sum(total * total, axis=(0, 1), keepdims=True), (8, 128))
    arrive(share(lambda p: e1.at[me1], e1, me1, peers1, on1))
    e2[me2] = add_slots(e1, n1)
    arrive(share(lambda p: e2.at[me2], e2, me2, peers2, on2))
    e3[me3] = add_slots(e2, n2)
    arrive(share(lambda p: e3.at[me3], e3, me3, peers3, on3))
    store(e3, e_out)
    arrive(p2_copies + p3_copies)
    net.finish()
    for copy in stores:
        copy.wait()


def finish_kernel(raws, outs, ins, results, in_sem, out_sem):
    loads = [pltpu.make_async_copy(src, dst, in_sem.at[k]) for k, (src, dst) in enumerate(zip(raws, ins))]
    for load in loads:
        load.start()
    new1t, p2, sq2, p3, sq3, core_t, e3 = ins
    out2, out3, out_core, out_e = results
    finals = [pltpu.make_async_copy(src, dst, out_sem.at[k]) for k, (src, dst) in enumerate(zip((new1t,) + results, outs))]
    loads[1].wait()
    loads[2].wait()
    out2[...] = p2[...].reshape(out2.shape) / jnp.sqrt(add_slots(sq2, sq2.shape[0])[:1])
    finals[1].start()
    loads[3].wait()
    loads[4].wait()
    out3[...] = p3[...].reshape(out3.shape) / jnp.sqrt(add_slots(sq3, sq3.shape[0])[:1])
    finals[2].start()
    loads[0].wait()
    finals[0].start()
    loads[5].wait()
    width = out_core.shape[2]
    for a in range(out_core.shape[0]):
        out_core[a] = core_t[:, a * width : (a + 1) * width]
    finals[3].start()
    loads[6].wait()
    out_e[...] = add_slots(e3, e3.shape[0])[:1, :1]
    finals[4].start()
    for final in finals:
        final.wait()


def solution(mesh):
    n1, n2, n3 = mesh.shape["a1"], mesh.shape["a2"], mesh.shape["a3"]
    nx = n1 // 2

    def local_sweep(tensor, u_time, u_height, u_width):
        fl, hl, wl = tensor.shape
        rank1 = u_time.shape[1]
        half, cz, cy, c1w, hr = fl // 2, 128 // n3, 128 // n3 // n2, 128 // n3 // n1, hl // n1
        ar, bq, wx, zq = rank1 // n1, 128 // n2, wl // 2 // nx, n3 // n2
        hops = n3 - 1
        frames, parts = n1 * fl, hl // 2 // n3 // 8
        outs = [(rank1, frames), (hl, 128), (n2, 8, 128), (wl, 128), (n3, 8, 128), (cz, 256), (n3, 8, 128)]
        scratch = [
            (tensor.shape, BF16), ((rank1, frames), F32), (u_height.shape, F32), (u_width.shape, F32), ((wl, 128), F32), *[(shape, F32) for shape in outs],
            ((256, 256), BF16), ((frames, 128), BF16), ((n3, fl, cz, hl), F32), ((2, hops, 2, half, cz // 2, hl), F32),
            ((fl, cz, hl), BF16), ((cz, fl, hl), BF16), ((n1, hr, fl, wl), BF16), ((hr, frames, wl), BF16), ((c1w, frames, hl), BF16),
            ((cz, fl, 128), F32), ((n2, cy, fl, 128), F32), ((fl, cy * 128), BF16), ((n1, fl, cy * 128), BF16), ((fl, frames), F32),
            ((n2, fl, 128), F32), ((n3, fl, 128), F32), ((n2, fl, 128), F32), ((n1, fl, 128), F32),
            ((c1w * rank1, hl), BF16), ((n2, c1w * rank1, hl), BF16), ((hr, rank1, wl), BF16), ((rank1, hr, wl), BF16), ((ar, hl, wl), BF16),
            ((2, n2, hl // 2, hl), F32), ((n2, hl // 2, hl), F32), ((n2, n3, parts, 8, hl), F32), ((parts, nx, n3, 8, hl), F32),
            ((n3, parts, 8, hl), F32), ((parts, n3, 8, hl), F32),
            ((nx, hl // 2 // n3, 128), F32), ((n3, hl // 2 // n3, 128), F32), ((2, hl // 2, 128), F32),
            ((n2, ar, bq, wl), F32), ((n2, ar, bq, wl), F32), ((ar * bq, wl), BF16), ((n3, ar * bq, wl), BF16),
            ((2, n3, wl // 2, wl), F32), ((n3, wl // 2, wl), F32), ((nx, n3, wx, wl), F32), ((nx, n3, wx, wl), F32),
            ((n3, wx, wl), F32), ((n2, zq, wx, wl), F32),
            ((n2, wx, 128), F32), ((nx, wx, 128), F32), ((2, wl // 2, 128), F32),
            ((n3, cz, 256), F32), ((n3, cz, 256), F32), ((n1, 8, 128), F32), ((n2, 8, 128), F32),
        ]
        raws = list(outs)
        raws[1], raws[3] = (n2, hl, 128), (n3, wl, 128)
        raw = pl.pallas_call(
            functools.partial(sweep_kernel, n1, n2, n3),
            out_shape=[jax.ShapeDtypeStruct(shape, F32) for shape in raws],
            in_specs=[pl.BlockSpec(memory_space=pl.ANY)] * 4,
            out_specs=[pl.BlockSpec(memory_space=pl.ANY)] * 7,
            scratch_shapes=[pltpu.VMEM(shape, dtype) for shape, dtype in scratch]
            + [pltpu.SemaphoreType.DMA((256,)), pltpu.SemaphoreType.DMA((256,)), pltpu.SemaphoreType.DMA((6,)), pltpu.SemaphoreType.DMA((8,))],
            compiler_params=pltpu.CompilerParams(collective_id=0, has_side_effects=True, vmem_limit_bytes=60 * 1024 * 1024),
            name="sweep",
        )(tensor, u_time.T, u_height, u_width)
        shapes = [(rank1, frames), u_height.shape, u_width.shape, (ar, cz, bq), (1, 1)]
        new1t, new2, new3, core_t, energy = pl.pallas_call(
            lambda *refs: finish_kernel(refs[:7], refs[7:12], refs[12:19], refs[19:23], *refs[23:]),
            out_shape=[jax.ShapeDtypeStruct(shape, F32) for shape in shapes],
            in_specs=[pl.BlockSpec(memory_space=pl.ANY)] * 7,
            out_specs=[pl.BlockSpec(memory_space=pl.ANY)] * 5,
            scratch_shapes=[pltpu.VMEM(shape, F32) for shape in raws + shapes[1:]]
            + [pltpu.SemaphoreType.DMA((7,)), pltpu.SemaphoreType.DMA((5,))],
            compiler_params=pltpu.CompilerParams(vmem_limit_bytes=60 * 1024 * 1024),
            name="finish",
        )(*raw)
        return new1t.T, new2, new3, core_t.transpose(0, 2, 1), energy.reshape(())

    return jax.shard_map(
        local_sweep,
        mesh=mesh,
        in_specs=(P("a1", "a2", "a3"), P(), P(), P()),
        out_specs=(P(), P(), P(), P("a1", "a2", "a3"), P()),
        check_vma=False,
    )
```

```python
import functools

import jax
import jax.numpy as jnp
from jax import lax
from jax.experimental import pallas as pl
from jax.experimental.pallas import tpu as pltpu
from jax.sharding import PartitionSpec as P

F32 = jnp.float32
BF16 = jnp.bfloat16
MESH = pl.DeviceIdType.MESH
EXCHANGES = 82
NN = ((1,), (0,))
NT = ((1,), (1,))
TN = ((0,), (0,))


def dot(a, b, dims=NN):
    return lax.dot_general(a, b, (dims, ((), ())), preferred_element_type=F32)


class Net:
    def __init__(self, send_sem, recv_sem, near):
        self.send_sem, self.recv_sem, self.near, self.exchanges = send_sem, recv_sem, near, []

    def describe(self, k, src, dst, device):
        return pltpu.make_async_remote_copy(
            src_ref=src, dst_ref=dst, send_sem=self.send_sem.at[k], recv_sem=self.recv_sem.at[k], device_id=device, device_id_type=MESH
        )

    def exchange(self, copies, span):
        k = len(self.exchanges)
        for src, dst, device in copies:
            self.describe(k, src, dst, device).start()
        self.exchanges.append(self.describe(k, span, span, self.near))
        return self.exchanges[-1]

    def send(self, src, dst, device):
        return self.exchange([(src, dst, device)], dst)

    def finish(self):
        for exchange in self.exchanges:
            exchange.wait_send()


def arrive(exchanges):
    for exchange in exchanges:
        exchange.wait_recv()


def add_slots(buf, count):
    total = buf[0]
    for k in range(1, count):
        total = total + buf[k]
    return total


def swap16(perm, block):
    n = block.shape[-1]
    return dot(perm, block.reshape(256, n)).astype(BF16).reshape(16, 16, n)


def sweep_kernel(
    n1, n2, n3,
    x_hbm, u1_hbm, u2_hbm, u3_hbm,
    new1t_out, p2_out, sq2_out, p3_out, sq3_out, core_out, e_out,
    x, u1, u2, u3, u3_here, new1t, p2, sq2, p3, sq3, out_core, e3,
    perm, u1p, tp, rin, rin_b, tb, tt, xp, xr, t2,
    y1p, y1y, y1b, y1a, gp1, g1y, g1z, p1y, p1a,
    y2o, y2y, z1, z2, zf, gp2, b0, g0, b1, g1, b2, p2x, p2z, p2c,
    y3p, y3y, y3o, y3z, gp3, c0, h0, c1, h1, c2, p3y, p3x, p3c,
    cp, cpz, e1,
    send_sem, recv_sem, load_sem, store_sem,
):
    me1, me2, me3 = lax.axis_index("a1"), lax.axis_index("a2"), lax.axis_index("a3")
    core, mex, nx = lax.rem(me1, 2), me1 // 2, n1 // 2
    fl, hl, wl = x.shape
    net = Net(send_sem, recv_sem, {"a3": lax.rem(me3 + 1, n3)})
    stores = []

    def store(src, dst):
        stores.append(pltpu.make_async_copy(src, dst, store_sem.at[len(stores)]))
        stores[-1].start()


    def peers(me, n):
        return [lax.rem(me + d, n) for d in range(1, n)]

    peers1, peers2, peers3, peersx = peers(me1, n1), peers(me2, n2), peers(me3, n3), peers(mex, nx)

    def share(src, buf, me, ps, device):
        return [net.exchange([(src(p), buf.at[me], device(p)) for p in ps], buf.at[pl.ds(0, len(ps))])]

    def on1(p):
        return {"a1": p}

    def on2(p):
        return {"a2": p}

    def on3(p):
        return {"a3": p}

    def onx(p):
        return {"a1": 2 * p + core}

    other = {"a1": 2 * mex + 1 - core}

    barrier = pltpu.get_barrier_semaphore()
    for ps, device in ((peers3, on3), (peers2, on2), (peers1, on1)):
        for p in ps:
            pl.semaphore_signal(barrier, inc=1, device_id=device(p), device_id_type=MESH)

    half = fl // 3 * 2
    width_here = pl.ds(pl.multiple_of(me3 * wl, wl), wl)
    loads = [
        pltpu.make_async_copy(src, dst, load_sem.at[k])
        for k, (src, dst) in enumerate(
            [
                (u3_hbm.at[width_here], u3_here),
                (x_hbm.at[pl.ds(0, half)], x.at[pl.ds(0, half)]),
                (x_hbm.at[pl.ds(half, fl - half)], x.at[pl.ds(half, fl - half)]),
                (u1_hbm, u1),
                (u2_hbm, u2),
                (u3_hbm, u3),
            ]
        )
    ]
    for load in loads:
        load.start()

    for p in peers2:
        for q in peers1:
            pl.semaphore_signal(barrier, inc=1, device_id={"a2": p, "a1": q}, device_id_type=MESH)

    row = lax.broadcasted_iota(jnp.int32, (256, 256), 0)
    col = lax.broadcasted_iota(jnp.int32, (256, 256), 1)
    perm[...] = jnp.where(col == lax.rem(row, 16) * 16 + row // 16, 1.0, 0.0).astype(BF16)

    cz = tp.shape[2]
    reach = n3 // 2
    loads[0].wait()
    u3t = u3_here[...].T.astype(BF16)

    def t_frame(i, carry):
        tp[:, i] = dot(u3t, x[i], NT).reshape(n3, cz, hl)
        return carry

    hops, ch = n3 - 1, cz // 2
    cuts = ((0, half), (half, fl - half))
    rins = (rin, rin_b)
    way_step = (1, n3 - 1)

    def t_part(way, sub, root):
        return tp.at[root, pl.ds(*cuts[sub]), pl.ds(way * ch, ch)]

    def root_at(way, step):
        return lax.rem(me3 + n3 - step, n3) if way == 0 else lax.rem(me3 + step, n3)

    ring = {}

    def send_piece(way, sub, step):
        ring[way, sub, step] = net.send(
            t_part(way, sub, root_at(way, step)), rins[sub].at[way, step - 1], on3(lax.rem(me3 + way_step[way], n3))
        )

    loads[1].wait()
    lax.fori_loop(0, half, t_frame, 0, unroll=4)
    pl.semaphore_wait(barrier, n1 * n2 + n3 - 2)
    send_piece(0, 0, 1)
    send_piece(1, 0, 1)
    loads[2].wait()
    lax.fori_loop(half, fl, t_frame, 0, unroll=4)
    send_piece(0, 1, 1)
    send_piece(1, 1, 1)

    hr = hl // n1

    def x_slice(r):
        for hh in range(0, hr, 16):
            for g in range(0, fl, 16):
                rows = pl.ds(pl.multiple_of(r * hr + hh, 16), 16)
                xp[r, hh : hh + 16, g : g + 16, :] = swap16(perm[...], x[g : g + 16, rows, :])

    frames_here = pl.ds(pl.multiple_of(me1 * fl, fl), fl)
    def x_moves():
        for p in peers1:
            x_slice(p)
            yield xp.at[p], xr.at[:, frames_here, :], on1(p)

    x_copies = [net.exchange(x_moves(), xr.at[:, pl.ds(0, (n1 - 1) * fl), :])]
    x_slice(me1)
    xr[:, frames_here, :] = xp[me1]
    for load in loads[3:]:
        load.wait()
    rank1 = u1.shape[0]
    u1p[:, :rank1] = u1[...].T.astype(BF16)
    u1p[:, rank1:] = jnp.zeros((u1p.shape[0], 128 - rank1), BF16)

    u2_here = u2[pl.ds(pl.multiple_of(me2 * hl, hl), hl), :].astype(BF16)
    cy, c1w = cz // n2, cz // n1
    y1_copies = []

    def t_done(sub):
        first, count = cuts[sub]
        total = [t_part(way, sub, me3)[...] + rins[sub][way, hops - 1] for way in (0, 1)]
        tb[first : first + count] = jnp.concatenate(total, axis=1).astype(BF16)
        for g in range(first, first + count, 16):
            tt[:, g : g + 16, :] = swap16(perm[...], tb[g : g + 16])
        frames = pl.ds(first, count)
        y1p[:, frames, :] = dot(tt[:, frames, :].reshape(cz * count, hl), u2_here).reshape(cz, count, 128)
        moves = [(y1p.at[pl.ds(p * cy, cy), frames], y1y.at[me2, :, frames], on2(p)) for p in peers2]
        y1_copies.append(net.exchange(moves, y1y.at[pl.ds(0, n2 - 1), :, frames]))
        y1y[me2, :, frames] = y1p[pl.ds(me2 * cy, cy), frames]

    for step in range(1, n3):
        for sub in (0, 1):
            for way in (0, 1):
                arrive([ring[way, sub, step]])
                if step < hops:
                    mine = t_part(way, sub, root_at(way, step + 1))
                    mine[...] = mine[...] + rins[sub][way, step - 1]
                    send_piece(way, sub, step + 1)
            if step == hops:
                t_done(sub)
    t_moves = [(tt.at[pl.ds(p * c1w, c1w)], t2.at[:, frames_here, :], on1(p)) for p in peers1]
    t_copies = [net.exchange(t_moves, t2.at[:, pl.ds(0, (n1 - 1) * fl), :])]
    t2[:, frames_here, :] = tt[pl.ds(me1 * c1w, c1w)]
    arrive(y1_copies)
    lane = lax.broadcasted_iota(jnp.int32, (cy, fl, 128), 2)
    width = 128 // n2
    y1 = None
    for q in range(n2):
        for side, turn in ((0, 1), (1, n2 - 1)):
            chain = y1y[(q + turn) % n2]
            for k in range(2, n2 + 1):
                chain = chain + y1y[(q + turn * k) % n2]
            y1 = chain if y1 is None else jnp.where(lane >= q * width + side * (width // 2), chain, y1)
    y1 = y1.astype(BF16)
    for c in range(cy):
        y1b[:, c * 128 : (c + 1) * 128] = y1[c]

    y1_all = share(lambda p: y1b, y1a, me1, peers1, on1)
    y1a[me1] = y1b[...]
    arrive(y1_all)
    gp1[...] = dot(y1b[...], y1a[...].reshape(n1 * fl, cy * 128), NT)
    tiles_c = gp1.shape[1] // 128

    def cols_of(p):
        return pl.ds(pl.multiple_of(lax.rem(p, tiles_c) * 128, 128), 128)

    copies = share(lambda p: gp1.at[:, cols_of(p)], g1y, me2, peers2, on2)
    g1y[me2] = gp1[:, cols_of(me2)]
    arrive(copies)
    g1z[me3] = add_slots(g1y, n2)
    arrive(share(lambda p: g1z.at[me3], g1z, me3, peers3, on3))
    gram = add_slots(g1z, n3).astype(BF16)
    p1y[me2] = dot(gram, u1p[cols_of(me2), :])
    arrive(share(lambda p: p1y.at[me2], p1y, me2, peers2, on2))
    p1a[me1] = add_slots(p1y, tiles_c)
    arrive(share(lambda p: p1a.at[me1], p1a, me1, peers1, on1))
    power = p1a[...].reshape(n1 * fl, 128).T[:rank1]
    new1 = power / jnp.sqrt(jnp.sum(power * power, axis=1, keepdims=True))
    new1t[...] = new1
    store(new1t, new1t_out)
    u1t = new1.astype(BF16)

    arrive(t_copies)
    for c in range(c1w):
        y2o[c * rank1 : (c + 1) * rank1] = dot(u1t, t2[c]).astype(BF16)
    y2y[me2] = y2o[...]
    y2_copies = share(lambda p: y2o, y2y, me2, peers2, on2)

    arrive(x_copies)
    for h in range(hr):
        z1[h] = dot(u1t, xr[h]).astype(BF16)
    for hh in range(0, hr, 16):
        for g in range(0, rank1, 16):
            z2[g : g + 16, hh : hh + 16, :] = swap16(perm[...], z1[hh : hh + 16, g : g + 16, :])
    ar = rank1 // n1
    z_rows = pl.ds(pl.multiple_of(me1 * hr, hr), hr)
    z_moves = [(z2.at[pl.ds(p * ar, ar)], zf.at[:, z_rows, :], on1(p)) for p in peers1]
    z_copies = [net.exchange(z_moves, zf.at[:, pl.ds(0, (n1 - 1) * hr), :])]
    zf[:, z_rows, :] = z2[pl.ds(me1 * ar, ar)]

    arrive(y2_copies)
    for q in range(n2):
        gp2[:, q] = dot(y2o[...], y2y[q], TN).reshape(2, hl // 2, hl)
    swap = net.send(gp2.at[1 - core], b0, other)
    arrive([swap])
    g0[...] = (gp2[core] + b0[...]).reshape(g0.shape)
    pieces2 = []
    parts = hl // 2 // n3 // 8
    for k in range(parts):
        b1[k, mex] = g0[mex, :, k]
        pieces_x = share(lambda p: g0.at[p, :, k], b1.at[k], mex, peersx, onx)
        pieces2.append(pieces_x)
    pieces_z = []
    for k in range(parts):
        arrive(pieces2[k])
        g1[:, k] = add_slots(b1.at[k], nx)
        pieces_z += share(lambda p: g1.at[p, k], b2.at[k], me3, peers3, on3)
        b2[k, me3] = g1[me3, k]
    arrive(pieces_z)
    gram = jnp.concatenate([add_slots(b2.at[k], n3) for k in range(parts)], axis=0).astype(BF16)
    p2x[mex] = dot(gram, u2[pl.ds(pl.multiple_of(mex * hl, hl), hl), :].astype(BF16))
    arrive(share(lambda p: p2x.at[mex], p2x, mex, peersx, onx))
    p2z[me3] = add_slots(p2x, nx)
    arrive(share(lambda p: p2z.at[me3], p2z, me3, peers3, on3))
    p2c[core] = p2z[...].reshape(hl // 2, 128)
    arrive([net.send(p2c.at[core], p2c.at[core], other)])
    power = p2c[...].reshape(hl, 128)
    sq2[me2] = jnp.broadcast_to(jnp.sum(power * power, axis=0, keepdims=True), (8, 128))
    p2[...] = power
    store(p2, p2_out.at[me2])
    copies = share(lambda p: sq2.at[me2], sq2, me2, peers2, on2)
    arrive(copies)
    store(sq2, sq2_out)
    norm2 = jnp.sqrt(add_slots(sq2, n2)[:1])
    u2t = (power / norm2).T.astype(BF16)

    arrive(z_copies)
    bq = 128 // n2
    for a in range(ar):
        y3p[:, a] = dot(u2t, zf[a]).reshape(n2, bq, wl)
    copies = share(lambda p: y3p.at[p], y3y, me2, peers2, on2)
    p2_copies = share(lambda p: p2, p2_out, me2, peers2, on2)
    y3y[me2] = y3p[me2]
    arrive(copies)
    y3o[...] = add_slots(y3y, n2).astype(BF16).reshape(ar * bq, wl)

    wx = wl // 2 // nx
    order = [d for k in range(1, reach) for d in (k, n3 - k)] + [reach]
    peer_of = {d: lax.rem(me3 + d, n3) for d in order}
    y3z[me3] = y3o[...]
    incoming = {n3 - d: net.send(y3o, y3z.at[me3], on3(peer_of[d])) for d in order}
    groups = [[0, 1, n3 - 1], [2, n3 - 2], [3, n3 - 3, 4]]
    pieces_x = []
    for group in groups:
        swaps = []
        for d in group:
            if d:
                arrive([incoming[d]])
            q = peer_of[d] if d else me3
            gp3[:, q] = dot(y3o[...], y3z[q], TN).reshape(2, wl // 2, wl)
            swaps.append((q, net.send(gp3.at[1 - core, q], c0.at[q], other)))
        for q, swap in swaps:
            arrive([swap])
            h0[:, q] = (gp3[core, q] + c0[q]).reshape(nx, wx, wl)
            c1[mex, q] = h0[mex, q]
            pieces_x.append(net.exchange([(h0.at[p, q], c1.at[mex, q], onx(p)) for p in peersx], c1.at[pl.ds(0, nx - 1), 0]))
    arrive(pieces_x)
    h1[...] = add_slots(c1, nx)
    zq = n3 // n2
    copies = share(lambda p: h1.at[pl.ds(p * zq, zq)], c2, me2, peers2, on2)
    c2[me2] = h1[pl.ds(me2 * zq, zq)]
    arrive(copies)
    gram = add_slots(c2, n2).astype(BF16)
    power = jnp.zeros((wx, 128), F32)
    for q in range(zq):
        power = power + dot(gram[q], u3[pl.ds(pl.multiple_of((me2 * zq + q) * wl, wl), wl), :].astype(BF16))
    p3y[me2] = power
    arrive(share(lambda p: p3y.at[me2], p3y, me2, peers2, on2))
    p3x[mex] = add_slots(p3y, n2)
    arrive(share(lambda p: p3x.at[mex], p3x, mex, peersx, onx))
    p3c[core] = p3x[...].reshape(wl // 2, 128)
    arrive([net.send(p3c.at[core], p3c.at[core], other)])
    power = p3c[...].reshape(wl, 128)
    sq3[me3] = jnp.broadcast_to(jnp.sum(power * power, axis=0, keepdims=True), (8, 128))
    p3[...] = power
    store(p3, p3_out.at[me3])
    copies = share(lambda p: sq3.at[me3], sq3, me3, peers3, on3)
    arrive(copies)
    store(sq3, sq3_out)
    norm3 = jnp.sqrt(add_slots(sq3, n3)[:1])
    u3n = (power / norm3).T.astype(BF16)

    kk = ar * bq
    cp[...] = jnp.zeros_like(cp)
    cp[:, :, :kk] = dot(u3n, y3o[...], NT).reshape(n3, cz, kk)
    copies = share(lambda p: cp.at[p], cpz, me3, peers3, on3)
    p3_copies = share(lambda p: p3, p3_out, me3, peers3, on3)
    cpz[me3] = cp[me3]
    arrive(copies)
    total = add_slots(cpz, n3)
    out_core[...] = total
    store(out_core, core_out)
    mine = me2 * n1 + me1
    e1[mine] = jnp.broadcast_to(jnp.sum(total * total, axis=(0, 1), keepdims=True), (8, 128))
    e_moves = []
    for d2 in range(n2):
        for d1 in range(n1):
            if d1 or d2:
                e_moves.append((e1.at[mine], e1.at[mine], {"a2": lax.rem(me2 + d2, n2), "a1": lax.rem(me1 + d1, n1)}))
    arrive([net.exchange(e_moves, e1.at[pl.ds(0, n1 * n2 - 1)])])
    e3[me3] = add_slots(e1, n1 * n2)
    arrive(share(lambda p: e3.at[me3], e3, me3, peers3, on3))
    store(e3, e_out)
    arrive(p2_copies + p3_copies)
    net.finish()
    for copy in stores:
        copy.wait()


def finish_kernel(raws, outs, ins, results, in_sem, out_sem):
    loads = [pltpu.make_async_copy(src, dst, in_sem.at[k]) for k, (src, dst) in enumerate(zip(raws, ins))]
    for load in loads:
        load.start()
    new1t, p2, sq2, p3, sq3, core_t, e3 = ins
    out2, out3, out_core, out_e = results
    finals = [pltpu.make_async_copy(src, dst, out_sem.at[k]) for k, (src, dst) in enumerate(zip((new1t,) + results, outs))]
    loads[1].wait()
    loads[2].wait()
    out2[...] = p2[...].reshape(out2.shape) / jnp.sqrt(add_slots(sq2, sq2.shape[0])[:1])
    finals[1].start()
    loads[3].wait()
    loads[4].wait()
    out3[...] = p3[...].reshape(out3.shape) / jnp.sqrt(add_slots(sq3, sq3.shape[0])[:1])
    finals[2].start()
    loads[0].wait()
    finals[0].start()
    loads[5].wait()
    width = out_core.shape[2]
    for a in range(out_core.shape[0]):
        out_core[a] = core_t[:, a * width : (a + 1) * width]
    finals[3].start()
    loads[6].wait()
    out_e[...] = add_slots(e3, e3.shape[0])[:1, :1]
    finals[4].start()
    for final in finals:
        final.wait()


def solution(mesh):
    n1, n2, n3 = mesh.shape["a1"], mesh.shape["a2"], mesh.shape["a3"]
    nx = n1 // 2

    def local_sweep(tensor, u_time, u_height, u_width):
        fl, hl, wl = tensor.shape
        rank1 = u_time.shape[1]
        half, cz, cy, c1w, hr = fl // 3 * 2, 128 // n3, 128 // n3 // n2, 128 // n3 // n1, hl // n1
        ar, bq, wx, zq = rank1 // n1, 128 // n2, wl // 2 // nx, n3 // n2
        hops = n3 - 1
        frames, parts = n1 * fl, hl // 2 // n3 // 8
        outs = [(rank1, frames), (hl, 128), (n2, 8, 128), (wl, 128), (n3, 8, 128), (cz, 256), (n3, 8, 128)]
        scratch = [
            (tensor.shape, BF16), ((rank1, frames), F32), (u_height.shape, F32), (u_width.shape, F32), ((wl, 128), F32), *[(shape, F32) for shape in outs],
            ((256, 256), BF16), ((frames, 128), BF16), ((n3, fl, cz, hl), F32), ((2, hops, half, cz // 2, hl), F32), ((2, hops, fl - half, cz // 2, hl), F32),
            ((fl, cz, hl), BF16), ((cz, fl, hl), BF16), ((n1, hr, fl, wl), BF16), ((hr, frames, wl), BF16), ((c1w, frames, hl), BF16),
            ((cz, fl, 128), F32), ((n2, cy, fl, 128), F32), ((fl, cy * 128), BF16), ((n1, fl, cy * 128), BF16), ((fl, frames), F32),
            ((n2, fl, 128), F32), ((n3, fl, 128), F32), ((n2, fl, 128), F32), ((n1, fl, 128), F32),
            ((c1w * rank1, hl), BF16), ((n2, c1w * rank1, hl), BF16), ((hr, rank1, wl), BF16), ((rank1, hr, wl), BF16), ((ar, hl, wl), BF16),
            ((2, n2, hl // 2, hl), F32), ((n2, hl // 2, hl), F32), ((n2, n3, parts, 8, hl), F32), ((parts, nx, n3, 8, hl), F32),
            ((n3, parts, 8, hl), F32), ((parts, n3, 8, hl), F32),
            ((nx, hl // 2 // n3, 128), F32), ((n3, hl // 2 // n3, 128), F32), ((2, hl // 2, 128), F32),
            ((n2, ar, bq, wl), F32), ((n2, ar, bq, wl), F32), ((ar * bq, wl), BF16), ((n3, ar * bq, wl), BF16),
            ((2, n3, wl // 2, wl), F32), ((n3, wl // 2, wl), F32), ((nx, n3, wx, wl), F32), ((nx, n3, wx, wl), F32),
            ((n3, wx, wl), F32), ((n2, zq, wx, wl), F32),
            ((n2, wx, 128), F32), ((nx, wx, 128), F32), ((2, wl // 2, 128), F32),
            ((n3, cz, 256), F32), ((n3, cz, 256), F32), ((n2 * n1, 8, 128), F32),
        ]
        raws = list(outs)
        raws[1], raws[3] = (n2, hl, 128), (n3, wl, 128)
        raw = pl.pallas_call(
            functools.partial(sweep_kernel, n1, n2, n3),
            out_shape=[jax.ShapeDtypeStruct(shape, F32) for shape in raws],
            in_specs=[pl.BlockSpec(memory_space=pl.ANY)] * 4,
            out_specs=[pl.BlockSpec(memory_space=pl.ANY)] * 7,
            scratch_shapes=[pltpu.VMEM(shape, dtype) for shape, dtype in scratch]
            + [pltpu.SemaphoreType.DMA((EXCHANGES,)), pltpu.SemaphoreType.DMA((EXCHANGES,)), pltpu.SemaphoreType.DMA((6,)), pltpu.SemaphoreType.DMA((7,))],
            compiler_params=pltpu.CompilerParams(collective_id=0, has_side_effects=True, vmem_limit_bytes=60 * 1024 * 1024),
            name="sweep",
        )(tensor, u_time.T, u_height, u_width)
        shapes = [(rank1, frames), u_height.shape, u_width.shape, (ar, cz, bq), (1, 1)]
        new1t, new2, new3, core_t, energy = pl.pallas_call(
            lambda *refs: finish_kernel(refs[:7], refs[7:12], refs[12:19], refs[19:23], *refs[23:]),
            out_shape=[jax.ShapeDtypeStruct(shape, F32) for shape in shapes],
            in_specs=[pl.BlockSpec(memory_space=pl.ANY)] * 7,
            out_specs=[pl.BlockSpec(memory_space=pl.ANY)] * 5,
            scratch_shapes=[pltpu.VMEM(shape, F32) for shape in raws + shapes[1:]]
            + [pltpu.SemaphoreType.DMA((7,)), pltpu.SemaphoreType.DMA((5,))],
            compiler_params=pltpu.CompilerParams(vmem_limit_bytes=60 * 1024 * 1024),
            name="finish",
        )(*raw)
        return new1t.T, new2, new3, core_t.transpose(0, 2, 1), energy.reshape(())

    return jax.shard_map(
        local_sweep,
        mesh=mesh,
        in_specs=(P("a1", "a2", "a3"), P(), P(), P()),
        out_specs=(P(), P(), P(), P("a1", "a2", "a3"), P()),
        check_vma=False,
    )
```

```python
import functools

import jax
import jax.numpy as jnp
from jax import lax
from jax.experimental import pallas as pl
from jax.experimental.pallas import tpu as pltpu
from jax.sharding import PartitionSpec as P

F32 = jnp.float32
BF16 = jnp.bfloat16
MESH = pl.DeviceIdType.MESH
EXCHANGES = 83
NN = ((1,), (0,))
NT = ((1,), (1,))
TN = ((0,), (0,))


def dot(a, b, dims=NN):
    return lax.dot_general(a, b, (dims, ((), ())), preferred_element_type=F32)


class Net:
    def __init__(self, send_sem, recv_sem, near):
        self.send_sem, self.recv_sem, self.near, self.exchanges = send_sem, recv_sem, near, []

    def describe(self, k, src, dst, device):
        return pltpu.make_async_remote_copy(
            src_ref=src, dst_ref=dst, send_sem=self.send_sem.at[k], recv_sem=self.recv_sem.at[k], device_id=device, device_id_type=MESH
        )

    def exchange(self, copies, span):
        k = len(self.exchanges)
        for src, dst, device in copies:
            self.describe(k, src, dst, device).start()
        self.exchanges.append(self.describe(k, span, span, self.near))
        return self.exchanges[-1]

    def send(self, src, dst, device):
        return self.exchange([(src, dst, device)], dst)

    def finish(self):
        for exchange in self.exchanges:
            exchange.wait_send()


def arrive(exchanges):
    for exchange in exchanges:
        exchange.wait_recv()


def add_slots(buf, count):
    total = buf[0]
    for k in range(1, count):
        total = total + buf[k]
    return total


def swap16(perm, block):
    n = block.shape[-1]
    return dot(perm, block.reshape(256, n)).astype(BF16).reshape(16, 16, n)


def sweep_kernel(
    n1, n2, n3,
    x_hbm, u1_hbm, u2_hbm, u3_hbm,
    new1t_out, p2_out, sq2_out, p3_out, sq3_out, core_out, e_out,
    x, u1, u2, u3, u3_here, new1t, p2, sq2, sq3, out_core, e3,
    perm, u1p, tp, rin, rin_b, tb, tt, xp, xr, t2,
    y1p, y1y, y1b, y1a, gp1, g1y, g1z, p1y, p1a,
    y2o, y2y, z1, z2, zf, gp2, b0, g0, b1, g1, b2, p2x, p2z, p2c,
    y3p, y3y, y3o, y3z, gp3, c0, h0, c1, h1, c2, p3y, p3x, p3c,
    cp, cpz, e1,
    send_sem, recv_sem, load_sem, store_sem,
):
    me1, me2, me3 = lax.axis_index("a1"), lax.axis_index("a2"), lax.axis_index("a3")
    core, mex, nx = lax.rem(me1, 2), me1 // 2, n1 // 2
    fl, hl, wl = x.shape
    net = Net(send_sem, recv_sem, {"a3": lax.rem(me3 + 1, n3)})
    stores = []

    def store(src, dst):
        stores.append(pltpu.make_async_copy(src, dst, store_sem.at[len(stores)]))
        stores[-1].start()


    def peers(me, n):
        return [lax.rem(me + d, n) for d in range(1, n)]

    peers1, peers2, peers3, peersx = peers(me1, n1), peers(me2, n2), peers(me3, n3), peers(mex, nx)

    def share(src, buf, me, ps, device):
        return [net.exchange([(src(p), buf.at[me], device(p)) for p in ps], buf.at[pl.ds(0, len(ps))])]

    def on1(p):
        return {"a1": p}

    def on2(p):
        return {"a2": p}

    def on3(p):
        return {"a3": p}

    def onx(p):
        return {"a1": 2 * p + core}

    other = {"a1": 2 * mex + 1 - core}

    barrier = pltpu.get_barrier_semaphore()
    for ps, device in ((peers3, on3), (peers2, on2), (peers1, on1)):
        for p in ps:
            pl.semaphore_signal(barrier, inc=1, device_id=device(p), device_id_type=MESH)

    half = fl // 3 * 2
    width_here = pl.ds(pl.multiple_of(me3 * wl, wl), wl)
    loads = [
        pltpu.make_async_copy(src, dst, load_sem.at[k])
        for k, (src, dst) in enumerate(
            [
                (u3_hbm.at[width_here], u3_here),
                (x_hbm.at[pl.ds(0, half)], x.at[pl.ds(0, half)]),
                (x_hbm.at[pl.ds(half, fl - half)], x.at[pl.ds(half, fl - half)]),
                (u1_hbm, u1),
                (u2_hbm, u2),
                (u3_hbm, u3),
            ]
        )
    ]
    for load in loads:
        load.start()

    for p in peers2:
        for q in peers1:
            pl.semaphore_signal(barrier, inc=1, device_id={"a2": p, "a1": q}, device_id_type=MESH)

    row = lax.broadcasted_iota(jnp.int32, (256, 256), 0)
    col = lax.broadcasted_iota(jnp.int32, (256, 256), 1)
    perm[...] = jnp.where(col == lax.rem(row, 16) * 16 + row // 16, 1.0, 0.0).astype(BF16)

    cz = tp.shape[2]
    reach = n3 // 2
    loads[0].wait()
    u3t = u3_here[...].T.astype(BF16)

    def t_frame(i, carry):
        tp[:, i] = dot(u3t, x[i], NT).reshape(n3, cz, hl)
        return carry

    hops, ch = n3 - 1, cz // 2
    cuts = ((0, half), (half, fl - half))
    rins = (rin, rin_b)
    way_step = (1, n3 - 1)

    def t_part(way, sub, root):
        return tp.at[root, pl.ds(*cuts[sub]), pl.ds(way * ch, ch)]

    def root_at(way, step):
        return lax.rem(me3 + n3 - step, n3) if way == 0 else lax.rem(me3 + step, n3)

    ring = {}

    def send_piece(way, sub, step):
        ring[way, sub, step] = net.send(
            t_part(way, sub, root_at(way, step)), rins[sub].at[way, step - 1], on3(lax.rem(me3 + way_step[way], n3))
        )

    loads[1].wait()
    lax.fori_loop(0, half, t_frame, 0, unroll=4)
    pl.semaphore_wait(barrier, n1 * n2 + n3 - 2)
    send_piece(0, 0, 1)
    send_piece(1, 0, 1)
    loads[2].wait()
    lax.fori_loop(half, fl, t_frame, 0, unroll=4)
    send_piece(0, 1, 1)
    send_piece(1, 1, 1)

    hr = hl // n1

    def x_slice(r):
        for hh in range(0, hr, 16):
            for g in range(0, fl, 16):
                rows = pl.ds(pl.multiple_of(r * hr + hh, 16), 16)
                xp[r, hh : hh + 16, g : g + 16, :] = swap16(perm[...], x[g : g + 16, rows, :])

    frames_here = pl.ds(pl.multiple_of(me1 * fl, fl), fl)
    def x_moves():
        for p in peers1:
            x_slice(p)
            yield xp.at[p], xr.at[:, frames_here, :], on1(p)

    x_copies = [net.exchange(x_moves(), xr.at[:, pl.ds(0, (n1 - 1) * fl), :])]
    x_slice(me1)
    xr[:, frames_here, :] = xp[me1]
    for load in loads[3:]:
        load.wait()
    rank1 = u1.shape[0]
    u1p[:, :rank1] = u1[...].T.astype(BF16)
    u1p[:, rank1:] = jnp.zeros((u1p.shape[0], 128 - rank1), BF16)

    u2_here = u2[pl.ds(pl.multiple_of(me2 * hl, hl), hl), :].astype(BF16)
    cy, c1w = cz // n2, cz // n1
    y1_copies = []

    def t_done(sub):
        first, count = cuts[sub]
        total = [t_part(way, sub, me3)[...] + rins[sub][way, hops - 1] for way in (0, 1)]
        tb[first : first + count] = jnp.concatenate(total, axis=1).astype(BF16)
        for g in range(first, first + count, 16):
            tt[:, g : g + 16, :] = swap16(perm[...], tb[g : g + 16])
        frames = pl.ds(first, count)
        y1p[:, frames, :] = dot(tt[:, frames, :].reshape(cz * count, hl), u2_here).reshape(cz, count, 128)
        moves = [(y1p.at[pl.ds(p * cy, cy), frames], y1y.at[me2, :, frames], on2(p)) for p in peers2]
        y1_copies.append(net.exchange(moves, y1y.at[pl.ds(0, n2 - 1), :, frames]))
        y1y[me2, :, frames] = y1p[pl.ds(me2 * cy, cy), frames]

    for step in range(1, n3):
        for sub in (0, 1):
            for way in (0, 1):
                arrive([ring[way, sub, step]])
                if step < hops:
                    mine = t_part(way, sub, root_at(way, step + 1))
                    mine[...] = mine[...] + rins[sub][way, step - 1]
                    send_piece(way, sub, step + 1)
            if step == hops:
                t_done(sub)
    t_moves = [(tt.at[pl.ds(p * c1w, c1w)], t2.at[:, frames_here, :], on1(p)) for p in peers1]
    t_copies = [net.exchange(t_moves, t2.at[:, pl.ds(0, (n1 - 1) * fl), :])]
    t2[:, frames_here, :] = tt[pl.ds(me1 * c1w, c1w)]
    arrive(y1_copies)
    lane = lax.broadcasted_iota(jnp.int32, (cy, fl, 128), 2)
    width = 128 // n2
    y1 = None
    for q in range(n2):
        for side, turn in ((0, 1), (1, n2 - 1)):
            chain = y1y[(q + turn) % n2]
            for k in range(2, n2 + 1):
                chain = chain + y1y[(q + turn * k) % n2]
            y1 = chain if y1 is None else jnp.where(lane >= q * width + side * (width // 2), chain, y1)
    y1 = y1.astype(BF16)
    for c in range(cy):
        y1b[:, c * 128 : (c + 1) * 128] = y1[c]

    y1_all = share(lambda p: y1b, y1a, me1, peers1, on1)
    y1a[me1] = y1b[...]
    arrive(y1_all)
    gp1[...] = dot(y1b[...], y1a[...].reshape(n1 * fl, cy * 128), NT)
    tiles_c = gp1.shape[1] // 128

    def cols_of(p):
        return pl.ds(pl.multiple_of(lax.rem(p, tiles_c) * 128, 128), 128)

    copies = share(lambda p: gp1.at[:, cols_of(p)], g1y, me2, peers2, on2)
    g1y[me2] = gp1[:, cols_of(me2)]
    arrive(copies)
    g1z[me3] = add_slots(g1y, n2)
    arrive(share(lambda p: g1z.at[me3], g1z, me3, peers3, on3))
    gram = add_slots(g1z, n3).astype(BF16)
    p1y[me2] = dot(gram, u1p[cols_of(me2), :])
    arrive(share(lambda p: p1y.at[me2], p1y, me2, peers2, on2))
    p1a[me1] = add_slots(p1y, tiles_c)
    arrive(share(lambda p: p1a.at[me1], p1a, me1, peers1, on1))
    power = p1a[...].reshape(n1 * fl, 128).T[:rank1]
    new1 = power / jnp.sqrt(jnp.sum(power * power, axis=1, keepdims=True))
    new1t[...] = new1
    store(new1t, new1t_out)
    u1t = new1.astype(BF16)

    arrive(t_copies)
    for c in range(c1w):
        y2o[c * rank1 : (c + 1) * rank1] = dot(u1t, t2[c]).astype(BF16)
    y2y[me2] = y2o[...]
    y2_copies = share(lambda p: y2o, y2y, me2, peers2, on2)

    arrive(x_copies)
    for h in range(hr):
        z1[h] = dot(u1t, xr[h]).astype(BF16)
    for hh in range(0, hr, 16):
        for g in range(0, rank1, 16):
            z2[g : g + 16, hh : hh + 16, :] = swap16(perm[...], z1[hh : hh + 16, g : g + 16, :])
    ar = rank1 // n1
    z_rows = pl.ds(pl.multiple_of(me1 * hr, hr), hr)
    z_moves = [(z2.at[pl.ds(p * ar, ar)], zf.at[:, z_rows, :], on1(p)) for p in peers1]
    z_copies = [net.exchange(z_moves, zf.at[:, pl.ds(0, (n1 - 1) * hr), :])]
    zf[:, z_rows, :] = z2[pl.ds(me1 * ar, ar)]

    arrive(y2_copies)
    for q in range(n2):
        gp2[:, q] = dot(y2o[...], y2y[q], TN).reshape(2, hl // 2, hl)
    swap = net.send(gp2.at[1 - core], b0, other)
    arrive([swap])
    g0[...] = (gp2[core] + b0[...]).reshape(g0.shape)
    pieces2 = []
    parts = hl // 2 // n3 // 8
    for k in range(parts):
        b1[k, mex] = g0[mex, :, k]
        pieces_x = share(lambda p: g0.at[p, :, k], b1.at[k], mex, peersx, onx)
        pieces2.append(pieces_x)
    pieces_z = []
    for k in range(parts):
        arrive(pieces2[k])
        g1[:, k] = add_slots(b1.at[k], nx)
        pieces_z += share(lambda p: g1.at[p, k], b2.at[k], me3, peers3, on3)
        b2[k, me3] = g1[me3, k]
    arrive(pieces_z)
    gram = jnp.concatenate([add_slots(b2.at[k], n3) for k in range(parts)], axis=0).astype(BF16)
    p2x[mex] = dot(gram, u2[pl.ds(pl.multiple_of(mex * hl, hl), hl), :].astype(BF16))
    arrive(share(lambda p: p2x.at[mex], p2x, mex, peersx, onx))
    p2z[me3] = add_slots(p2x, nx)
    arrive(share(lambda p: p2z.at[me3], p2z, me3, peers3, on3))
    p2c[core] = p2z[...].reshape(hl // 2, 128)
    arrive([net.send(p2c.at[core], p2c.at[core], other)])
    power = p2c[...].reshape(hl, 128)
    sq2[me2] = jnp.broadcast_to(jnp.sum(power * power, axis=0, keepdims=True), (8, 128))
    p2[...] = power
    store(p2, p2_out.at[me2])
    copies = share(lambda p: sq2.at[me2], sq2, me2, peers2, on2)
    arrive(copies)
    store(sq2, sq2_out)
    norm2 = jnp.sqrt(add_slots(sq2, n2)[:1])
    u2t = (power / norm2).T.astype(BF16)

    arrive(z_copies)
    bq = 128 // n2
    for a in range(ar):
        y3p[:, a] = dot(u2t, zf[a]).reshape(n2, bq, wl)
    copies = share(lambda p: y3p.at[p], y3y, me2, peers2, on2)
    p2_copies = share(lambda p: p2, p2_out, me2, peers2, on2)
    y3y[me2] = y3p[me2]
    arrive(copies)
    y3o[...] = add_slots(y3y, n2).astype(BF16).reshape(ar * bq, wl)

    wx = wl // 2 // nx
    order = [d for k in range(1, reach) for d in (k, n3 - k)] + [reach]
    peer_of = {d: lax.rem(me3 + d, n3) for d in order}
    y3z[me3] = y3o[...]
    incoming = {n3 - d: net.send(y3o, y3z.at[me3], on3(peer_of[d])) for d in order}
    groups = [[0, 1, n3 - 1], [2, n3 - 2], [3, n3 - 3, 4]]
    pieces_x = []
    for group in groups:
        swaps = []
        for d in group:
            if d:
                arrive([incoming[d]])
            q = peer_of[d] if d else me3
            gp3[:, q] = dot(y3o[...], y3z[q], TN).reshape(2, wl // 2, wl)
            swaps.append((q, net.send(gp3.at[1 - core, q], c0.at[q], other)))
        for q, swap in swaps:
            arrive([swap])
            h0[:, q] = (gp3[core, q] + c0[q]).reshape(nx, wx, wl)
            c1[mex, q] = h0[mex, q]
            pieces_x.append(net.exchange([(h0.at[p, q], c1.at[mex, q], onx(p)) for p in peersx], c1.at[pl.ds(0, nx - 1), 0]))
    arrive(pieces_x)
    h1[...] = add_slots(c1, nx)
    zq = n3 // n2
    copies = share(lambda p: h1.at[pl.ds(p * zq, zq)], c2, me2, peers2, on2)
    c2[me2] = h1[pl.ds(me2 * zq, zq)]
    arrive(copies)
    gram = add_slots(c2, n2).astype(BF16)
    power = jnp.zeros((wx, 128), F32)
    for q in range(zq):
        power = power + dot(gram[q], u3[pl.ds(pl.multiple_of((me2 * zq + q) * wl, wl), wl), :].astype(BF16))
    p3y[me2] = power
    arrive(share(lambda p: p3y.at[me2], p3y, me2, peers2, on2))
    p3x[mex] = add_slots(p3y, n2)
    arrive(share(lambda p: p3x.at[mex], p3x, mex, peersx, onx))
    p3c[core] = p3x[...].reshape(wl // 2, 128)
    arrive([net.send(p3c.at[core], p3c.at[core], other)])
    power = p3c[...].reshape(wl, 128)
    sq3[me3] = jnp.broadcast_to(jnp.sum(power * power, axis=0, keepdims=True), (8, 128))
    store(p3c, p3_out.at[me3])
    copies = share(lambda p: sq3.at[me3], sq3, me3, peers3, on3)
    arrive(copies)
    store(sq3, sq3_out)
    norm3 = jnp.sqrt(add_slots(sq3, n3)[:1])
    u3n = (power / norm3).T.astype(BF16)

    kk = ar * bq
    cp[...] = jnp.zeros_like(cp)
    cp[:, :, :kk] = dot(u3n, y3o[...], NT).reshape(n3, cz, kk)
    copies = share(lambda p: cp.at[p], cpz, me3, peers3, on3)
    p3_moves = [(p3c.at[core], p3_out.at[me3, core], on3(p)) for p in peers3]
    p3_half = net.exchange(p3_moves, p3_out.at[pl.ds(0, n3 - 1), 0])
    cpz[me3] = cp[me3]
    arrive(copies)
    total = add_slots(cpz, n3)
    out_core[...] = total
    store(out_core, core_out)
    mine = me2 * n1 + me1
    e1[mine] = jnp.broadcast_to(jnp.sum(total * total, axis=(0, 1), keepdims=True), (8, 128))
    e_moves = []
    for d2 in range(n2):
        for d1 in range(n1):
            if d1 or d2:
                e_moves.append((e1.at[mine], e1.at[mine], {"a2": lax.rem(me2 + d2, n2), "a1": lax.rem(me1 + d1, n1)}))
    arrive([net.exchange(e_moves, e1.at[pl.ds(0, n1 * n2 - 1)])])
    e3[me3] = add_slots(e1, n1 * n2)
    e_last = share(lambda p: e3.at[me3], e3, me3, peers3, on3)
    arrive([p3_half])
    p3_moves = [(p3_out.at[p, core], p3_out.at[p, core], other) for p in peers3]
    p3_copies = [net.exchange(p3_moves, p3_out.at[pl.ds(0, n3 - 1), 0])]
    arrive(e_last)
    store(e3, e_out)
    arrive(p2_copies + p3_copies)
    net.finish()
    for copy in stores:
        copy.wait()


def finish_kernel(raws, outs, ins, results, in_sem, out_sem):
    loads = [pltpu.make_async_copy(src, dst, in_sem.at[k]) for k, (src, dst) in enumerate(zip(raws, ins))]
    for load in loads:
        load.start()
    new1t, p2, sq2, p3, sq3, core_t, e3 = ins
    out2, out3, out_core, out_e = results
    finals = [pltpu.make_async_copy(src, dst, out_sem.at[k]) for k, (src, dst) in enumerate(zip((new1t,) + results, outs))]
    loads[1].wait()
    loads[2].wait()
    out2[...] = p2[...].reshape(out2.shape) / jnp.sqrt(add_slots(sq2, sq2.shape[0])[:1])
    finals[1].start()
    loads[3].wait()
    loads[4].wait()
    out3[...] = p3[...].reshape(out3.shape) / jnp.sqrt(add_slots(sq3, sq3.shape[0])[:1])
    finals[2].start()
    loads[0].wait()
    finals[0].start()
    loads[5].wait()
    width = out_core.shape[2]
    for a in range(out_core.shape[0]):
        out_core[a] = core_t[:, a * width : (a + 1) * width]
    finals[3].start()
    loads[6].wait()
    out_e[...] = add_slots(e3, e3.shape[0])[:1, :1]
    finals[4].start()
    for final in finals:
        final.wait()


def solution(mesh):
    n1, n2, n3 = mesh.shape["a1"], mesh.shape["a2"], mesh.shape["a3"]
    nx = n1 // 2

    def local_sweep(tensor, u_time, u_height, u_width):
        fl, hl, wl = tensor.shape
        rank1 = u_time.shape[1]
        half, cz, cy, c1w, hr = fl // 3 * 2, 128 // n3, 128 // n3 // n2, 128 // n3 // n1, hl // n1
        ar, bq, wx, zq = rank1 // n1, 128 // n2, wl // 2 // nx, n3 // n2
        hops = n3 - 1
        frames, parts = n1 * fl, hl // 2 // n3 // 8
        outs = [(rank1, frames), (hl, 128), (n2, 8, 128), (n3, 8, 128), (cz, 256), (n3, 8, 128)]
        scratch = [
            (tensor.shape, BF16), ((rank1, frames), F32), (u_height.shape, F32), (u_width.shape, F32), ((wl, 128), F32), *[(shape, F32) for shape in outs],
            ((256, 256), BF16), ((frames, 128), BF16), ((n3, fl, cz, hl), F32), ((2, hops, half, cz // 2, hl), F32), ((2, hops, fl - half, cz // 2, hl), F32),
            ((fl, cz, hl), BF16), ((cz, fl, hl), BF16), ((n1, hr, fl, wl), BF16), ((hr, frames, wl), BF16), ((c1w, frames, hl), BF16),
            ((cz, fl, 128), F32), ((n2, cy, fl, 128), F32), ((fl, cy * 128), BF16), ((n1, fl, cy * 128), BF16), ((fl, frames), F32),
            ((n2, fl, 128), F32), ((n3, fl, 128), F32), ((n2, fl, 128), F32), ((n1, fl, 128), F32),
            ((c1w * rank1, hl), BF16), ((n2, c1w * rank1, hl), BF16), ((hr, rank1, wl), BF16), ((rank1, hr, wl), BF16), ((ar, hl, wl), BF16),
            ((2, n2, hl // 2, hl), F32), ((n2, hl // 2, hl), F32), ((n2, n3, parts, 8, hl), F32), ((parts, nx, n3, 8, hl), F32),
            ((n3, parts, 8, hl), F32), ((parts, n3, 8, hl), F32),
            ((nx, hl // 2 // n3, 128), F32), ((n3, hl // 2 // n3, 128), F32), ((2, hl // 2, 128), F32),
            ((n2, ar, bq, wl), F32), ((n2, ar, bq, wl), F32), ((ar * bq, wl), BF16), ((n3, ar * bq, wl), BF16),
            ((2, n3, wl // 2, wl), F32), ((n3, wl // 2, wl), F32), ((nx, n3, wx, wl), F32), ((nx, n3, wx, wl), F32),
            ((n3, wx, wl), F32), ((n2, zq, wx, wl), F32),
            ((n2, wx, 128), F32), ((nx, wx, 128), F32), ((2, wl // 2, 128), F32),
            ((n3, cz, 256), F32), ((n3, cz, 256), F32), ((n2 * n1, 8, 128), F32),
        ]
        raws = list(outs)
        raws[1] = (n2, hl, 128)
        raws.insert(3, (n3, 2, wl // 2, 128))
        raw = pl.pallas_call(
            functools.partial(sweep_kernel, n1, n2, n3),
            out_shape=[jax.ShapeDtypeStruct(shape, F32) for shape in raws],
            in_specs=[pl.BlockSpec(memory_space=pl.ANY)] * 4,
            out_specs=[pl.BlockSpec(memory_space=pl.ANY)] * 7,
            scratch_shapes=[pltpu.VMEM(shape, dtype) for shape, dtype in scratch]
            + [pltpu.SemaphoreType.DMA((EXCHANGES,)), pltpu.SemaphoreType.DMA((EXCHANGES,)), pltpu.SemaphoreType.DMA((6,)), pltpu.SemaphoreType.DMA((7,))],
            compiler_params=pltpu.CompilerParams(collective_id=0, has_side_effects=True, vmem_limit_bytes=60 * 1024 * 1024),
            name="sweep",
        )(tensor, u_time.T, u_height, u_width)
        shapes = [(rank1, frames), u_height.shape, u_width.shape, (ar, cz, bq), (1, 1)]
        new1t, new2, new3, core_t, energy = pl.pallas_call(
            lambda *refs: finish_kernel(refs[:7], refs[7:12], refs[12:19], refs[19:23], *refs[23:]),
            out_shape=[jax.ShapeDtypeStruct(shape, F32) for shape in shapes],
            in_specs=[pl.BlockSpec(memory_space=pl.ANY)] * 7,
            out_specs=[pl.BlockSpec(memory_space=pl.ANY)] * 5,
            scratch_shapes=[pltpu.VMEM(shape, F32) for shape in raws + shapes[1:]]
            + [pltpu.SemaphoreType.DMA((7,)), pltpu.SemaphoreType.DMA((5,))],
            compiler_params=pltpu.CompilerParams(vmem_limit_bytes=60 * 1024 * 1024),
            name="finish",
        )(*raw)
        return new1t.T, new2, new3, core_t.transpose(0, 2, 1), energy.reshape(())

    return jax.shard_map(
        local_sweep,
        mesh=mesh,
        in_specs=(P("a1", "a2", "a3"), P(), P(), P()),
        out_specs=(P(), P(), P(), P("a1", "a2", "a3"), P()),
        check_vma=False,
    )
```

```python
import functools

import jax
import jax.numpy as jnp
from jax import lax
from jax.experimental import pallas as pl
from jax.experimental.pallas import tpu as pltpu
from jax.sharding import PartitionSpec as P

F32 = jnp.float32
BF16 = jnp.bfloat16
MESH = pl.DeviceIdType.MESH
EXCHANGES = 91
NN = ((1,), (0,))
NT = ((1,), (1,))
TN = ((0,), (0,))


def dot(a, b, dims=NN):
    return lax.dot_general(a, b, (dims, ((), ())), preferred_element_type=F32)


class Net:
    def __init__(self, send_sem, recv_sem, near):
        self.send_sem, self.recv_sem, self.near, self.exchanges = send_sem, recv_sem, near, []

    def describe(self, k, src, dst, device):
        return pltpu.make_async_remote_copy(
            src_ref=src, dst_ref=dst, send_sem=self.send_sem.at[k], recv_sem=self.recv_sem.at[k], device_id=device, device_id_type=MESH
        )

    def exchange(self, copies, span):
        k = len(self.exchanges)
        for src, dst, device in copies:
            self.describe(k, src, dst, device).start()
        self.exchanges.append(self.describe(k, span, span, self.near))
        return self.exchanges[-1]

    def send(self, src, dst, device):
        return self.exchange([(src, dst, device)], dst)

    def finish(self):
        for exchange in self.exchanges:
            exchange.wait_send()


def arrive(exchanges):
    for exchange in exchanges:
        exchange.wait_recv()


def add_slots(buf, count):
    total = buf[0]
    for k in range(1, count):
        total = total + buf[k]
    return total


def swap16(perm, block):
    n = block.shape[-1]
    return dot(perm, block.reshape(256, n)).astype(BF16).reshape(16, 16, n)


def sweep_kernel(
    n1, n2, n3,
    x_hbm, u1_hbm, u2_hbm, u3_hbm,
    new1t_out, p2_out, sq2_out, p3_out, sq3_out, core_out, e_out,
    x, u1, u2, u3, u3_here, new1t, p2, sq2, sq3, out_core, e3,
    perm, u1p, tp, rin, rin_b, tb, tt, xp, xr, t2,
    y1p, y1y, y1b, y1a, gp1, g1y, g1z, p1y, p1a,
    y2o, y2y, z1, z2, zf, gp2, b0, g0, b1, g1, b2, p2x, p2z, p2c,
    y3p, y3y, y3o, y3z, gp3, c0, h0, c1, h1, c2, p3y, p3x, p3c,
    cp, cpz, e1,
    send_sem, recv_sem, load_sem, store_sem,
):
    me1, me2, me3 = lax.axis_index("a1"), lax.axis_index("a2"), lax.axis_index("a3")
    core, mex, nx = lax.rem(me1, 2), me1 // 2, n1 // 2
    fl, hl, wl = x.shape
    net = Net(send_sem, recv_sem, {"a3": lax.rem(me3 + 1, n3)})
    stores = []

    def store(src, dst):
        stores.append(pltpu.make_async_copy(src, dst, store_sem.at[len(stores)]))
        stores[-1].start()


    def peers(me, n):
        return [lax.rem(me + d, n) for d in range(1, n)]

    peers1, peers2, peers3, peersx = peers(me1, n1), peers(me2, n2), peers(me3, n3), peers(mex, nx)

    def share(src, buf, me, ps, device):
        return [net.exchange([(src(p), buf.at[me], device(p)) for p in ps], buf.at[pl.ds(0, len(ps))])]

    def on1(p):
        return {"a1": p}

    def on2(p):
        return {"a2": p}

    def on3(p):
        return {"a3": p}

    def onx(p):
        return {"a1": 2 * p + core}

    other = {"a1": 2 * mex + 1 - core}

    barrier = pltpu.get_barrier_semaphore()
    for ps, device in ((peers3, on3), (peers2, on2), (peers1, on1)):
        for p in ps:
            pl.semaphore_signal(barrier, inc=1, device_id=device(p), device_id_type=MESH)

    half = fl // 3 * 2
    width_here = pl.ds(pl.multiple_of(me3 * wl, wl), wl)
    loads = [
        pltpu.make_async_copy(src, dst, load_sem.at[k])
        for k, (src, dst) in enumerate(
            [
                (u3_hbm.at[width_here], u3_here),
                (x_hbm.at[pl.ds(0, half)], x.at[pl.ds(0, half)]),
                (x_hbm.at[pl.ds(half, fl - half)], x.at[pl.ds(half, fl - half)]),
                (u1_hbm, u1),
                (u2_hbm, u2),
                (u3_hbm, u3),
            ]
        )
    ]
    for load in loads:
        load.start()

    for p in peers2:
        for q in peers1:
            pl.semaphore_signal(barrier, inc=1, device_id={"a2": p, "a1": q}, device_id_type=MESH)

    row = lax.broadcasted_iota(jnp.int32, (256, 256), 0)
    col = lax.broadcasted_iota(jnp.int32, (256, 256), 1)
    perm[...] = jnp.where(col == lax.rem(row, 16) * 16 + row // 16, 1.0, 0.0).astype(BF16)

    cz = tp.shape[2]
    reach = n3 // 2
    loads[0].wait()
    u3t = u3_here[...].T.astype(BF16)

    def t_frame(i, carry):
        tp[:, i] = dot(u3t, x[i], NT).reshape(n3, cz, hl)
        return carry

    hops, ch = n3 - 1, cz // 2
    cuts = ((0, half), (half, fl - half))
    rins = (rin, rin_b)
    way_step = (1, n3 - 1)

    def t_part(way, sub, root):
        return tp.at[root, pl.ds(*cuts[sub]), pl.ds(way * ch, ch)]

    def root_at(way, step):
        return lax.rem(me3 + n3 - step, n3) if way == 0 else lax.rem(me3 + step, n3)

    ring = {}

    def send_piece(way, sub, step):
        ring[way, sub, step] = net.send(
            t_part(way, sub, root_at(way, step)), rins[sub].at[way, step - 1], on3(lax.rem(me3 + way_step[way], n3))
        )

    loads[1].wait()
    lax.fori_loop(0, half, t_frame, 0, unroll=4)
    pl.semaphore_wait(barrier, n1 * n2 + n3 - 2)
    send_piece(0, 0, 1)
    send_piece(1, 0, 1)
    loads[2].wait()
    lax.fori_loop(half, fl, t_frame, 0, unroll=4)
    send_piece(0, 1, 1)
    send_piece(1, 1, 1)

    hr = hl // n1

    def x_slice(r):
        for hh in range(0, hr, 16):
            for g in range(0, fl, 16):
                rows = pl.ds(pl.multiple_of(r * hr + hh, 16), 16)
                xp[r, hh : hh + 16, g : g + 16, :] = swap16(perm[...], x[g : g + 16, rows, :])

    frames_here = pl.ds(pl.multiple_of(me1 * fl, fl), fl)
    def x_moves():
        for p in peers1:
            x_slice(p)
            yield xp.at[p], xr.at[:, frames_here, :], on1(p)

    x_copies = [net.exchange(x_moves(), xr.at[:, pl.ds(0, (n1 - 1) * fl), :])]
    x_slice(me1)
    xr[:, frames_here, :] = xp[me1]
    for load in loads[3:]:
        load.wait()
    rank1 = u1.shape[0]
    u1p[:, :rank1] = u1[...].T.astype(BF16)
    u1p[:, rank1:] = jnp.zeros((u1p.shape[0], 128 - rank1), BF16)

    u2_here = u2[pl.ds(pl.multiple_of(me2 * hl, hl), hl), :].astype(BF16)
    cy, c1w = cz // n2, cz // n1
    y1_copies = []

    def t_done(sub):
        first, count = cuts[sub]
        total = [t_part(way, sub, me3)[...] + rins[sub][way, hops - 1] for way in (0, 1)]
        tb[first : first + count] = jnp.concatenate(total, axis=1).astype(BF16)
        for g in range(first, first + count, 16):
            tt[:, g : g + 16, :] = swap16(perm[...], tb[g : g + 16])
        frames = pl.ds(first, count)
        y1p[:, frames, :] = dot(tt[:, frames, :].reshape(cz * count, hl), u2_here).reshape(cz, count, 128)
        moves = [(y1p.at[pl.ds(p * cy, cy), frames], y1y.at[me2, :, frames], on2(p)) for p in peers2]
        y1_copies.append(net.exchange(moves, y1y.at[pl.ds(0, n2 - 1), :, frames]))
        y1y[me2, :, frames] = y1p[pl.ds(me2 * cy, cy), frames]

    for step in range(1, n3):
        for sub in (0, 1):
            for way in (0, 1):
                arrive([ring[way, sub, step]])
                if step < hops:
                    mine = t_part(way, sub, root_at(way, step + 1))
                    mine[...] = mine[...] + rins[sub][way, step - 1]
                    send_piece(way, sub, step + 1)
            if step == hops:
                t_done(sub)
    t_moves = [(tt.at[pl.ds(p * c1w, c1w)], t2.at[:, frames_here, :], on1(p)) for p in peers1]
    t_copies = [net.exchange(t_moves, t2.at[:, pl.ds(0, (n1 - 1) * fl), :])]
    t2[:, frames_here, :] = tt[pl.ds(me1 * c1w, c1w)]
    arrive(y1_copies)
    lane = lax.broadcasted_iota(jnp.int32, (cy, fl, 128), 2)
    width = 128 // n2
    y1 = None
    for q in range(n2):
        for side, turn in ((0, 1), (1, n2 - 1)):
            chain = y1y[(q + turn) % n2]
            for k in range(2, n2 + 1):
                chain = chain + y1y[(q + turn * k) % n2]
            y1 = chain if y1 is None else jnp.where(lane >= q * width + side * (width // 2), chain, y1)
    y1 = y1.astype(BF16)
    for c in range(cy):
        y1b[:, c * 128 : (c + 1) * 128] = y1[c]

    y1_all = share(lambda p: y1b, y1a, me1, peers1, on1)
    y1a[me1] = y1b[...]
    arrive(y1_all)
    gp1[...] = dot(y1b[...], y1a[...].reshape(n1 * fl, cy * 128), NT)
    tiles_c = gp1.shape[1] // 128

    def cols_of(p):
        return pl.ds(pl.multiple_of(lax.rem(p, tiles_c) * 128, 128), 128)

    copies = share(lambda p: gp1.at[:, cols_of(p)], g1y, me2, peers2, on2)
    g1y[me2] = gp1[:, cols_of(me2)]
    arrive(copies)
    g1z[me3] = add_slots(g1y, n2)
    arrive(share(lambda p: g1z.at[me3], g1z, me3, peers3, on3))
    gram = add_slots(g1z, n3).astype(BF16)
    p1y[me2] = dot(gram, u1p[cols_of(me2), :])
    arrive(share(lambda p: p1y.at[me2], p1y, me2, peers2, on2))
    p1a[me1] = add_slots(p1y, tiles_c)
    arrive(share(lambda p: p1a.at[me1], p1a, me1, peers1, on1))
    power = p1a[...].reshape(n1 * fl, 128).T[:rank1]
    new1 = power / jnp.sqrt(jnp.sum(power * power, axis=1, keepdims=True))
    new1t[...] = new1
    store(new1t, new1t_out)
    u1t = new1.astype(BF16)

    arrive(t_copies)
    for c in range(c1w):
        y2o[c * rank1 : (c + 1) * rank1] = dot(u1t, t2[c]).astype(BF16)
    y2y[me2] = y2o[...]
    y2_copies = share(lambda p: y2o, y2y, me2, peers2, on2)

    arrive(x_copies)
    for h in range(hr):
        z1[h] = dot(u1t, xr[h]).astype(BF16)
    for hh in range(0, hr, 16):
        for g in range(0, rank1, 16):
            z2[g : g + 16, hh : hh + 16, :] = swap16(perm[...], z1[hh : hh + 16, g : g + 16, :])
    ar = rank1 // n1
    z_rows = pl.ds(pl.multiple_of(me1 * hr, hr), hr)
    z_moves = [(z2.at[pl.ds(p * ar, ar)], zf.at[:, z_rows, :], on1(p)) for p in peers1]
    z_copies = [net.exchange(z_moves, zf.at[:, pl.ds(0, (n1 - 1) * hr), :])]
    zf[:, z_rows, :] = z2[pl.ds(me1 * ar, ar)]

    arrive(y2_copies)
    for q in range(n2):
        gp2[:, q] = dot(y2o[...], y2y[q], TN).reshape(2, hl // 2, hl)
    swap = net.send(gp2.at[1 - core], b0, other)
    arrive([swap])
    g0[...] = (gp2[core] + b0[...]).reshape(g0.shape)
    pieces2 = []
    parts = hl // 2 // n3 // 8
    for k in range(parts):
        b1[k, mex] = g0[mex, :, k]
        pieces_x = share(lambda p: g0.at[p, :, k], b1.at[k], mex, peersx, onx)
        pieces2.append(pieces_x)
    pieces_z = []
    for k in range(parts):
        arrive(pieces2[k])
        g1[:, k] = add_slots(b1.at[k], nx)
        pieces_z += share(lambda p: g1.at[p, k], b2.at[k], me3, peers3, on3)
        b2[k, me3] = g1[me3, k]
    arrive(pieces_z)
    gram = jnp.concatenate([add_slots(b2.at[k], n3) for k in range(parts)], axis=0).astype(BF16)
    p2x[mex] = dot(gram, u2[pl.ds(pl.multiple_of(mex * hl, hl), hl), :].astype(BF16))
    arrive(share(lambda p: p2x.at[mex], p2x, mex, peersx, onx))
    p2z[me3] = add_slots(p2x, nx)
    arrive(share(lambda p: p2z.at[me3], p2z, me3, peers3, on3))
    p2c[core] = p2z[...].reshape(hl // 2, 128)
    arrive([net.send(p2c.at[core], p2c.at[core], other)])
    power = p2c[...].reshape(hl, 128)
    sq2[me2] = jnp.broadcast_to(jnp.sum(power * power, axis=0, keepdims=True), (8, 128))
    p2[...] = power
    store(p2, p2_out.at[me2])
    copies = share(lambda p: sq2.at[me2], sq2, me2, peers2, on2)
    arrive(copies)
    store(sq2, sq2_out)
    norm2 = jnp.sqrt(add_slots(sq2, n2)[:1])
    u2t = (power / norm2).T.astype(BF16)

    arrive(z_copies)
    bq = 128 // n2
    for a in range(ar):
        y3p[:, a] = dot(u2t, zf[a]).reshape(n2, bq, wl)
    y3y[me2] = y3p[me2]
    ah = ar // 2
    y3_copies = []
    for a in (0, ah):
        now = pl.ds(a, ah)
        moves = [(y3p.at[p, now], y3y.at[me2, now], on2(p)) for p in peers2]
        y3_copies.append(net.exchange(moves, y3y.at[pl.ds(0, n2 - 1), now]))
    p2_copies = share(lambda p: p2, p2_out, me2, peers2, on2)

    wx = wl // 2 // nx
    order = [d for k in range(1, reach) for d in (k, n3 - k)] + [reach]
    peer_of = {d: lax.rem(me3 + d, n3) for d in order}
    incoming = {d: [] for d in order}
    for k, a in enumerate((0, ah)):
        arrive([y3_copies[k]])
        rows = pl.ds(a * bq, ah * bq)
        block = add_slots([y3y[q, a : a + ah] for q in range(n2)], n2).astype(BF16).reshape(ah * bq, wl)
        y3o[rows, :] = block
        y3z[me3, rows, :] = block
        for d in order:
            incoming[n3 - d].append(net.send(y3o.at[rows], y3z.at[me3, rows], on3(peer_of[d])))
    groups = [[0, 1, n3 - 1], [2, n3 - 2], [3, n3 - 3, 4]]
    pieces_x = []
    for group in groups:
        swaps = []
        for d in group:
            if d:
                arrive(incoming[d])
            q = peer_of[d] if d else me3
            gp3[:, q] = dot(y3o[...], y3z[q], TN).reshape(2, wl // 2, wl)
            swaps.append((q, net.send(gp3.at[1 - core, q], c0.at[q], other)))
        for q, swap in swaps:
            arrive([swap])
            h0[:, q] = (gp3[core, q] + c0[q]).reshape(nx, wx, wl)
            c1[mex, q] = h0[mex, q]
            pieces_x.append(net.exchange([(h0.at[p, q], c1.at[mex, q], onx(p)) for p in peersx], c1.at[pl.ds(0, nx - 1), 0]))
    arrive(pieces_x)
    h1[...] = add_slots(c1, nx)
    zq = n3 // n2
    copies = share(lambda p: h1.at[pl.ds(p * zq, zq)], c2, me2, peers2, on2)
    c2[me2] = h1[pl.ds(me2 * zq, zq)]
    arrive(copies)
    gram = add_slots(c2, n2).astype(BF16)
    power = jnp.zeros((wx, 128), F32)
    for q in range(zq):
        power = power + dot(gram[q], u3[pl.ds(pl.multiple_of((me2 * zq + q) * wl, wl), wl), :].astype(BF16))
    p3y[me2] = power
    arrive(share(lambda p: p3y.at[me2], p3y, me2, peers2, on2))
    p3x[mex] = add_slots(p3y, n2)
    arrive(share(lambda p: p3x.at[mex], p3x, mex, peersx, onx))
    p3c[core] = p3x[...].reshape(wl // 2, 128)
    arrive([net.send(p3c.at[core], p3c.at[core], other)])
    power = p3c[...].reshape(wl, 128)
    sq3[me3] = jnp.broadcast_to(jnp.sum(power * power, axis=0, keepdims=True), (8, 128))
    store(p3c, p3_out.at[me3])
    copies = share(lambda p: sq3.at[me3], sq3, me3, peers3, on3)
    arrive(copies)
    store(sq3, sq3_out)
    norm3 = jnp.sqrt(add_slots(sq3, n3)[:1])
    u3n = (power / norm3).T.astype(BF16)

    kk = ar * bq
    cp[...] = jnp.zeros_like(cp)
    cp[:, :, :kk] = dot(u3n, y3o[...], NT).reshape(n3, cz, kk)
    copies = share(lambda p: cp.at[p], cpz, me3, peers3, on3)
    p3_moves = [(p3c.at[core], p3_out.at[me3, core], on3(p)) for p in peers3]
    p3_half = net.exchange(p3_moves, p3_out.at[pl.ds(0, n3 - 1), 0])
    cpz[me3] = cp[me3]
    arrive(copies)
    total = add_slots(cpz, n3)
    out_core[...] = total
    store(out_core, core_out)
    mine = me2 * n1 + me1
    e1[mine] = jnp.broadcast_to(jnp.sum(total * total, axis=(0, 1), keepdims=True), (8, 128))
    e_moves = []
    for d2 in range(n2):
        for d1 in range(n1):
            if d1 or d2:
                e_moves.append((e1.at[mine], e1.at[mine], {"a2": lax.rem(me2 + d2, n2), "a1": lax.rem(me1 + d1, n1)}))
    arrive([net.exchange(e_moves, e1.at[pl.ds(0, n1 * n2 - 1)])])
    e3[me3] = add_slots(e1, n1 * n2)
    e_last = share(lambda p: e3.at[me3], e3, me3, peers3, on3)
    arrive([p3_half])
    p3_moves = [(p3_out.at[p, core], p3_out.at[p, core], other) for p in peers3]
    p3_copies = [net.exchange(p3_moves, p3_out.at[pl.ds(0, n3 - 1), 0])]
    arrive(e_last)
    store(e3, e_out)
    arrive(p2_copies + p3_copies)
    net.finish()
    for copy in stores:
        copy.wait()


def finish_kernel(raws, outs, ins, results, in_sem, out_sem):
    loads = [pltpu.make_async_copy(src, dst, in_sem.at[k]) for k, (src, dst) in enumerate(zip(raws, ins))]
    for load in loads:
        load.start()
    new1t, p2, sq2, p3, sq3, core_t, e3 = ins
    out2, out3, out_core, out_e = results
    finals = [pltpu.make_async_copy(src, dst, out_sem.at[k]) for k, (src, dst) in enumerate(zip((new1t,) + results, outs))]
    loads[1].wait()
    loads[2].wait()
    out2[...] = p2[...].reshape(out2.shape) / jnp.sqrt(add_slots(sq2, sq2.shape[0])[:1])
    finals[1].start()
    loads[3].wait()
    loads[4].wait()
    out3[...] = p3[...].reshape(out3.shape) / jnp.sqrt(add_slots(sq3, sq3.shape[0])[:1])
    finals[2].start()
    loads[0].wait()
    finals[0].start()
    loads[5].wait()
    width = out_core.shape[2]
    for a in range(out_core.shape[0]):
        out_core[a] = core_t[:, a * width : (a + 1) * width]
    finals[3].start()
    loads[6].wait()
    out_e[...] = add_slots(e3, e3.shape[0])[:1, :1]
    finals[4].start()
    for final in finals:
        final.wait()


def solution(mesh):
    n1, n2, n3 = mesh.shape["a1"], mesh.shape["a2"], mesh.shape["a3"]
    nx = n1 // 2

    def local_sweep(tensor, u_time, u_height, u_width):
        fl, hl, wl = tensor.shape
        rank1 = u_time.shape[1]
        half, cz, cy, c1w, hr = fl // 3 * 2, 128 // n3, 128 // n3 // n2, 128 // n3 // n1, hl // n1
        ar, bq, wx, zq = rank1 // n1, 128 // n2, wl // 2 // nx, n3 // n2
        hops = n3 - 1
        frames, parts = n1 * fl, hl // 2 // n3 // 8
        outs = [(rank1, frames), (hl, 128), (n2, 8, 128), (n3, 8, 128), (cz, 256), (n3, 8, 128)]
        scratch = [
            (tensor.shape, BF16), ((rank1, frames), F32), (u_height.shape, F32), (u_width.shape, F32), ((wl, 128), F32), *[(shape, F32) for shape in outs],
            ((256, 256), BF16), ((frames, 128), BF16), ((n3, fl, cz, hl), F32), ((2, hops, half, cz // 2, hl), F32), ((2, hops, fl - half, cz // 2, hl), F32),
            ((fl, cz, hl), BF16), ((cz, fl, hl), BF16), ((n1, hr, fl, wl), BF16), ((hr, frames, wl), BF16), ((c1w, frames, hl), BF16),
            ((cz, fl, 128), F32), ((n2, cy, fl, 128), F32), ((fl, cy * 128), BF16), ((n1, fl, cy * 128), BF16), ((fl, frames), F32),
            ((n2, fl, 128), F32), ((n3, fl, 128), F32), ((n2, fl, 128), F32), ((n1, fl, 128), F32),
            ((c1w * rank1, hl), BF16), ((n2, c1w * rank1, hl), BF16), ((hr, rank1, wl), BF16), ((rank1, hr, wl), BF16), ((ar, hl, wl), BF16),
            ((2, n2, hl // 2, hl), F32), ((n2, hl // 2, hl), F32), ((n2, n3, parts, 8, hl), F32), ((parts, nx, n3, 8, hl), F32),
            ((n3, parts, 8, hl), F32), ((parts, n3, 8, hl), F32),
            ((nx, hl // 2 // n3, 128), F32), ((n3, hl // 2 // n3, 128), F32), ((2, hl // 2, 128), F32),
            ((n2, ar, bq, wl), F32), ((n2, ar, bq, wl), F32), ((ar * bq, wl), BF16), ((n3, ar * bq, wl), BF16),
            ((2, n3, wl // 2, wl), F32), ((n3, wl // 2, wl), F32), ((nx, n3, wx, wl), F32), ((nx, n3, wx, wl), F32),
            ((n3, wx, wl), F32), ((n2, zq, wx, wl), F32),
            ((n2, wx, 128), F32), ((nx, wx, 128), F32), ((2, wl // 2, 128), F32),
            ((n3, cz, 256), F32), ((n3, cz, 256), F32), ((n2 * n1, 8, 128), F32),
        ]
        raws = list(outs)
        raws[1] = (n2, hl, 128)
        raws.insert(3, (n3, 2, wl // 2, 128))
        raw = pl.pallas_call(
            functools.partial(sweep_kernel, n1, n2, n3),
            out_shape=[jax.ShapeDtypeStruct(shape, F32) for shape in raws],
            in_specs=[pl.BlockSpec(memory_space=pl.ANY)] * 4,
            out_specs=[pl.BlockSpec(memory_space=pl.ANY)] * 7,
            scratch_shapes=[pltpu.VMEM(shape, dtype) for shape, dtype in scratch]
            + [pltpu.SemaphoreType.DMA((EXCHANGES,)), pltpu.SemaphoreType.DMA((EXCHANGES,)), pltpu.SemaphoreType.DMA((6,)), pltpu.SemaphoreType.DMA((7,))],
            compiler_params=pltpu.CompilerParams(collective_id=0, has_side_effects=True, vmem_limit_bytes=60 * 1024 * 1024),
            name="sweep",
        )(tensor, u_time.T, u_height, u_width)
        shapes = [(rank1, frames), u_height.shape, u_width.shape, (ar, cz, bq), (1, 1)]
        new1t, new2, new3, core_t, energy = pl.pallas_call(
            lambda *refs: finish_kernel(refs[:7], refs[7:12], refs[12:19], refs[19:23], *refs[23:]),
            out_shape=[jax.ShapeDtypeStruct(shape, F32) for shape in shapes],
            in_specs=[pl.BlockSpec(memory_space=pl.ANY)] * 7,
            out_specs=[pl.BlockSpec(memory_space=pl.ANY)] * 5,
            scratch_shapes=[pltpu.VMEM(shape, F32) for shape in raws + shapes[1:]]
            + [pltpu.SemaphoreType.DMA((7,)), pltpu.SemaphoreType.DMA((5,))],
            compiler_params=pltpu.CompilerParams(vmem_limit_bytes=60 * 1024 * 1024),
            name="finish",
        )(*raw)
        return new1t.T, new2, new3, core_t.transpose(0, 2, 1), energy.reshape(())

    return jax.shard_map(
        local_sweep,
        mesh=mesh,
        in_specs=(P("a1", "a2", "a3"), P(), P(), P()),
        out_specs=(P(), P(), P(), P("a1", "a2", "a3"), P()),
        check_vma=False,
    )
```
